128 devices in a mesh: row: 16 (over y, z), col: 8 (over x, core).
Axes of the slice: x: 4, y: 4, z: 4, core: 2. Of those that a mesh axis runs over, the one named last changes fastest.
Arguments:
- eigvec_halves: float32 [3072, 32768], P('col', 'row'), may hold values from -6 to 6
- rotation_mate: int32 [3072], replicated, may hold values from 0 to 3071, as said below
- givens_theta: float32 [3072], replicated, may hold values from -3.140625 to 3.140625
- kept_vectors: int32 [3072], replicated, may hold values from 0 to 3071, as said below
- secular_singularities: float32 [3072], replicated, may hold values from -0.25 to 3071.25, as said below
- secular_coefficients: float32 [3072], replicated, may hold values from -6 to 6
- secular_zeros: float32 [512], replicated, may hold values from 0.4 to 3071.6, as said below
Outputs:
- packed_vectors: float32 [3072, 32768], P(('row', 'col'))
- panel: float32 [512, 32768], P('col', 'row')
The draws below stay inside these ranges and needn't reach their ends.
Inputs may be any that keep to these rules, and one draw needn't show every extreme that they name: `rotation_mate`: partner is an involution. Column blocks of 384 belong to the indices of col in order; at most 24 columns of one block pair with columns of any one other block, exactly that many for some two blocks in every draw. `kept_vectors`: survivors is a permutation. Compacted positions form consecutive blocks of 24, one block per device of row+col in order; one block takes at most 4 columns from any one column block of 384, exactly that many from some. secular_singularities[k] lies within 0.25 of k. secular_zeros[j] lies within 0.1 of an integer plus 0.5, between j * K / 512 and (j + 1) * K / 512.
All inputs are finite; a program needn't handle non-finite values.
Results may differ from the reference program's by a relative error of at most 0.00007.
Values sent between devices are 32-bit elements; how exact they have to be, the bound alone decides.
No kernel may reach another device: no remote copies, remote signals or barrier semaphores. Data moves between devices by JAX's collectives and lax.ppermute only.
A program may use at most 64 MiB of HBM per device.

```python
import jax
import jax.numpy as jnp
from jax import lax

N = 32768
KD = 384
PANEL = 512
K = 3072
PAIR_CAP = 24
N_ROW = 16
N_COL = 8


def draw_rotation_mate(key, part):
    order_key, count_key = jax.random.split(jax.random.fold_in(key, 11))
    slot_order = jax.vmap(lambda subkey: jax.random.permutation(subkey, KD))(jax.random.split(order_key, N_COL)).astype(jnp.int32)
    counts = jax.random.randint(count_key, (N_COL, N_COL), PAIR_CAP // 2, PAIR_CAP + 1).astype(jnp.int32)
    counts = counts.at[1, 0].set(PAIR_CAP)
    device_ids = jnp.arange(N_COL, dtype=jnp.int32)[:, None]
    slot_ids = jnp.arange(N_COL * PAIR_CAP, dtype=jnp.int32)[None, :]
    round_ids = slot_ids // PAIR_CAP
    within = slot_ids % PAIR_CAP
    other_dev = (round_ids - device_ids) % N_COL
    limit = counts[round_ids, jnp.minimum(device_ids, other_dev)]
    twin_slot = within ^ 1
    same_dev = other_dev == device_ids
    active = jnp.where(same_dev, (within < limit) & (twin_slot < limit), within < limit)
    mate_slot = jnp.where(same_dev, round_ids * PAIR_CAP + twin_slot, slot_ids)
    mate_ids = other_dev * KD + slot_order[other_dev, mate_slot]
    local_labels = device_ids * KD + slot_order[device_ids, slot_ids]
    result = jnp.arange(K, dtype=jnp.int32)
    return result.at[local_labels.reshape(-1)].set(jnp.where(active, mate_ids, local_labels).reshape(-1))


def draw_kept_vectors(key, part):
    shift_key, own_key, place_key = jax.random.split(jax.random.fold_in(key, 23), 3)
    dest_count = N_ROW * N_COL
    every_destination = KD // N_ROW
    share_base = every_destination // N_COL
    share_extra = share_base // 3
    shifts = jax.random.permutation(shift_key, N_COL)[:2].astype(jnp.int32)
    source_ids = jnp.arange(N_COL, dtype=jnp.int32)[:, None]
    dest_ids = jnp.arange(dest_count, dtype=jnp.int32)[None, :]
    raised = ((source_ids + dest_ids + shifts[0]) % N_COL == 0).astype(jnp.int32)
    lowered = ((source_ids + dest_ids + shifts[1]) % N_COL == 0).astype(jnp.int32)
    load_table = share_base + share_extra * (raised - lowered)
    out_start = jnp.cumsum(load_table, axis=1) - load_table
    in_start = jnp.cumsum(load_table, axis=0) - load_table
    finish_table = in_start + load_table
    position_ids = jnp.arange(every_destination, dtype=jnp.int32)
    source_of = jnp.sum((finish_table.T[:, :, None] <= position_ids[None, None, :]).astype(jnp.int32), axis=1)
    offset_in = position_ids[None, :] - jnp.take_along_axis(in_start.T, source_of, axis=1)
    slot_here = jnp.take_along_axis(out_start.T, source_of, axis=1) + offset_in
    orders = jax.vmap(lambda subkey: jax.random.permutation(subkey, KD))(jax.random.split(own_key, N_COL)).astype(jnp.int32)
    column_ids = source_of * KD + orders[source_of, slot_here]
    shuffles = jax.vmap(lambda subkey: jax.random.permutation(subkey, every_destination))(jax.random.split(place_key, dest_count)).astype(jnp.int32)
    column_ids = jnp.take_along_axis(column_ids, shuffles, axis=1)
    return column_ids.reshape(-1).astype(jnp.int32)


def draw_secular_singularities(key, part):
    jitter_key = jax.random.fold_in(key, 31)
    base_ids = jnp.arange(K, dtype=jnp.float32)
    jitter = 0.1 * jnp.clip(jax.random.normal(jitter_key, (K,), jnp.float32), -2.5, 2.5)
    return base_ids + jitter


def draw_secular_zeros(key, part):
    placement_key, jitter_key = jax.random.split(jax.random.fold_in(key, 37))
    stride = K // PANEL
    offsets = jax.random.randint(placement_key, (PANEL,), 0, stride)
    centers = (jnp.arange(PANEL, dtype=jnp.int32) * stride + offsets).astype(jnp.float32) + 0.5
    jitter = 0.04 * jnp.clip(jax.random.normal(jitter_key, (PANEL,), jnp.float32), -2.5, 2.5)
    return centers + jitter


def shard_levels(rng, dims, cuts, low, high):
    def one(dim, shards_of):
        heights = jax.random.uniform(jax.random.fold_in(jax.random.fold_in(rng, 6), dim), (shards_of,), jnp.float32, low / len(cuts), high / len(cuts))
        return jnp.repeat(jnp.exp(heights), dims[dim] // shards_of).reshape((-1,) + (1,) * (len(dims) - dim - 1))

    gain = one(*cuts[0])
    for cut in cuts[1:]:
        gain = gain * one(*cut)
    return gain


def centred(key, extent, deviation, most, shards=(), held_as=jnp.bfloat16):
    values = deviation * jax.random.normal(key, extent, jnp.float32)
    if shards:
        values = values * shard_levels(key, extent, shards, -0.22, 0.18)
    return jnp.clip(values, -most, most).astype(held_as)


def setup_inputs(seed: int = 0) -> dict:
    seeds = jax.random.split(jax.random.key(seed), 8)
    return {
        "eigvec_halves": centred(seeds[0], (K, N), 1.0, 6.0, ((0, 8), (1, 16)), jnp.float32),
        "rotation_mate": draw_rotation_mate(jax.random.fold_in(seeds[7], 71), 0),
        "givens_theta": jnp.clip(jax.random.uniform(seeds[2], (K,), jnp.float32, -3.140625, 3.140625), -3.140625, 3.140625),
        "kept_vectors": draw_kept_vectors(jax.random.fold_in(seeds[7], 71), 0),
        "secular_singularities": draw_secular_singularities(jax.random.fold_in(seeds[7], 71), 0),
        "secular_coefficients": centred(seeds[5], (K,), 1.0, 6.0, (), jnp.float32),
        "secular_zeros": draw_secular_zeros(jax.random.fold_in(seeds[7], 71), 0),
    }


def reference(eigvec_halves, rotation_mate, givens_theta, kept_vectors, secular_singularities, secular_coefficients, secular_zeros):
    local_labels = jnp.arange(eigvec_halves.shape[0], dtype=jnp.int32)
    paired = rotation_mate != local_labels
    angles_here = givens_theta[jnp.minimum(local_labels, rotation_mate)]
    sign_flip = jnp.where(local_labels < rotation_mate, -1.0, 1.0).astype(jnp.float32)
    cosine = jnp.where(paired, jnp.cos(angles_here), 1.0)
    sine_term = jnp.where(paired, sign_flip * jnp.sin(angles_here), 0.0)
    spun_vectors = cosine[:, None] * eigvec_halves + sine_term[:, None] * eigvec_halves[rotation_mate]
    packed_vectors = spun_vectors[kept_vectors]
    cauchy_raw = secular_coefficients[:, None] / (secular_singularities[:, None] - secular_zeros[None, :])
    col_scale = lax.rsqrt(lax.optimization_barrier(jnp.sum(cauchy_raw * cauchy_raw, axis=0)) + 1e-06)
    cauchy = cauchy_raw * col_scale[None, :]
    panel = lax.dot_general(cauchy, packed_vectors, (((0,), (0,)), ((), ())), precision=lax.Precision.HIGHEST, preferred_element_type=jnp.float32)
    return (packed_vectors, panel)
```

```python
import functools

import jax
import jax.numpy as jnp
from jax import lax
from jax.experimental import pallas as pl
from jax.experimental.pallas import tpu as pltpu
from jax.sharding import PartitionSpec as P

LANES = 128
SUB = 8


def to_tiles(rows):
    count, width = rows.shape
    tiles = rows.reshape(count // SUB, SUB, width // LANES, LANES)
    return tiles.transpose(0, 2, 1, 3).reshape(count * width // LANES, LANES)


def from_tiles(tiles, count, width):
    rows = tiles.reshape(count // SUB, width // LANES, SUB, LANES)
    return rows.transpose(0, 2, 1, 3).reshape(count, width)


def pack_kernel(lane_tiles, local_rows, mate_ref, dest_ref, cos_ref, sin_ref,
                local_hbm, mates_hbm, out_ref, rows_ref, sems):
    split = local_rows * lane_tiles
    copies = [
        pltpu.make_async_copy(local_hbm, rows_ref.at[pl.ds(0, split)], sems.at[0]),
        pltpu.make_async_copy(
            mates_hbm, rows_ref.at[pl.ds(split, mates_hbm.shape[0])], sems.at[1]
        ),
    ]
    for copy in copies:
        copy.start()
    for copy in copies:
        copy.wait()
    tile_rows = lane_tiles * SUB

    def column(i, carry):
        own = (i // SUB) * tile_rows + i % SUB
        mate = mate_ref[i]
        dest = pl.multiple_of(dest_ref[i], SUB)
        cosine = cos_ref[i]
        sine = sin_ref[i]
        for part in range(lane_tiles // SUB):
            offset = part * SUB * SUB
            a = rows_ref[pl.ds(own + offset, SUB, SUB), :]
            b = rows_ref[pl.ds(mate + offset, SUB, SUB), :]
            out_ref[pl.ds(dest + part * SUB, SUB), :] = cosine * a + sine * b
        return carry

    lax.fori_loop(0, local_rows, column, 0, unroll=4)


def unpack_kernel(lane_tiles, sources, wanted, per_step, start_ref, in_ref, out_ref):
    slots = in_ref.shape[0] // per_step
    for k in range(wanted):
        start = pl.multiple_of(start_ref[k], SUB)
        for r in range(per_step):
            for part in range(lane_tiles // SUB):
                value = in_ref[pl.ds(start + r * slots + part * SUB, SUB), :]
                first = (r * lane_tiles + part * SUB) * SUB + k % SUB
                out_ref[k // SUB, pl.ds(first, SUB, SUB), :] = value


def one_hot_sum(match, values):
    return jnp.sum(jnp.where(match, values[None, :], jnp.zeros((), values.dtype)), axis=1)


def shards(
    eigvec_halves,
    rotation_mate,
    givens_theta,
    kept_vectors,
    secular_singularities,
    secular_coefficients,
    secular_zeros,
):
    col_count = lax.axis_size("col")
    row_count = lax.axis_size("row")
    chips = col_count // 2
    block_cols, block_rows = eigvec_halves.shape
    total_cols = rotation_mate.shape[0]
    panel_cols = secular_zeros.shape[0]
    pair_cap = block_cols // 16
    lane_tiles = block_rows // LANES
    dest_count = row_count * col_count
    every = total_cols // dest_count
    move_cap = every // col_count + every // col_count // 3
    col_index = lax.axis_index("col")
    chip, core = col_index // 2, col_index % 2
    first_col = col_index * block_cols

    order = jnp.arange(block_cols, dtype=jnp.int32)
    labels = first_col + order
    mates = lax.dynamic_slice_in_dim(rotation_mate, first_col, block_cols)
    owner = mates // block_cols
    same_owner = owner[:, None] == owner[None, :]
    send_rank = jnp.sum((same_owner & (order[None, :] < order[:, None])).astype(jnp.int32), axis=1)
    send_slot = jnp.where(owner != col_index, owner * pair_cap + send_rank, -1)
    slots = jnp.arange(col_count * pair_cap, dtype=jnp.int32)
    pick = (slots[:, None] == send_slot[None, :]).astype(jnp.float32)
    outgoing = jnp.dot(
        pick, eigvec_halves, precision=lax.Precision.HIGHEST, preferred_element_type=jnp.float32
    ).reshape(col_count, pair_cap, block_rows)
    incoming = lax.all_to_all(outgoing, "col", split_axis=0, concat_axis=0, tiled=True)
    flat_in = incoming.reshape(col_count * pair_cap, block_rows)

    paired = mates != labels
    own_match = kept_vectors[None, :] == labels[:, None]
    mate_match = kept_vectors[None, :] == mates[:, None]
    positions = jnp.arange(total_cols, dtype=jnp.int32)
    spot = one_hot_sum(own_match, positions)
    pole = one_hot_sum(own_match, secular_singularities)
    weight = one_hot_sum(own_match, secular_coefficients)
    mate_pole = one_hot_sum(mate_match, secular_singularities)
    mate_weight = one_hot_sum(mate_match, secular_coefficients)
    angle = one_hot_sum(positions[None, :] == jnp.minimum(labels, mates)[:, None], givens_theta)
    sign_flip = jnp.where(labels < mates, -1.0, 1.0).astype(jnp.float32)
    cosine = jnp.where(paired, jnp.cos(angle), 1.0)
    sine = jnp.where(paired, sign_flip * jnp.sin(angle), 0.0)

    recv_rank = jnp.sum((same_owner & (mates[None, :] < mates[:, None])).astype(jnp.int32), axis=1)
    mate_row = jnp.where(
        owner != col_index, block_cols + owner * pair_cap + recv_rank, mates - first_col
    )
    mate_start = (mate_row // SUB) * (lane_tiles * SUB) + mate_row % SUB
    dest = spot // every
    dest_rank = jnp.sum(
        ((dest[:, None] == dest[None, :]) & (spot[None, :] < spot[:, None])).astype(jnp.int32),
        axis=1,
    )
    dest_start = (dest * move_cap + dest_rank) * lane_tiles

    parcels = pl.pallas_call(
        functools.partial(pack_kernel, lane_tiles, block_cols),
        out_shape=jax.ShapeDtypeStruct((dest_count * move_cap * lane_tiles, LANES), jnp.float32),
        in_specs=[pl.BlockSpec(memory_space=pltpu.SMEM)] * 4
        + [pl.BlockSpec(memory_space=pl.ANY)] * 2,
        out_specs=pl.BlockSpec(memory_space=pltpu.VMEM),
        scratch_shapes=[
            pltpu.VMEM(((block_cols + col_count * pair_cap) * lane_tiles, LANES), jnp.float32),
            pltpu.SemaphoreType.DMA((2,)),
        ],
        name="rotate_pack",
    )(mate_start, dest_start, cosine, sine, to_tiles(eigvec_halves), to_tiles(flat_in))
    arrived = lax.all_to_all(
        parcels.reshape(dest_count, move_cap * lane_tiles, LANES),
        ("row", "col"), split_axis=0, concat_axis=0, tiled=True,
    )

    raw = secular_coefficients[:, None] / (secular_singularities[:, None] - secular_zeros[None, :])
    scale_all = lax.rsqrt(jnp.sum(raw * raw, axis=0) + 1e-06)
    by_chip = jnp.stack([secular_zeros, scale_all]).reshape(2, chips, 2, panel_cols // col_count)
    by_chip = jnp.concatenate([by_chip, by_chip], axis=1)
    by_chip = lax.dynamic_slice_in_dim(by_chip, chip, chips, axis=1)

    def partial_panel(parity):
        mine = lax.dynamic_slice_in_dim(by_chip, parity, 1, axis=2).reshape(2, panel_cols // 2)
        zeros, scale = mine[0], mine[1]
        spun = (
            cosine[:, None] * (weight[:, None] / (pole[:, None] - zeros[None, :]))
            - sine[:, None] * (mate_weight[:, None] / (mate_pole[:, None] - zeros[None, :]))
        ) * scale[None, :]
        return lax.dot_general(
            spun, eigvec_halves, (((0,), (0,)), ((), ())),
            precision=lax.Precision.HIGH, preferred_element_type=jnp.float32,
        )

    def shift(array, chip_step):
        pairs = [
            (2 * x + c, 2 * ((x + chip_step) % chips) + c) for x in range(chips) for c in range(2)
        ]
        return lax.ppermute(array, "col", pairs)

    swap = [(c, c ^ 1) for c in range(col_count)]
    partner = lax.ppermute(partial_panel(1 - core), "col", swap)
    both = (partial_panel(core) + partner).reshape(chips, panel_cols // col_count, block_rows)
    half = panel_cols // col_count // 2
    far_up = shift(both[2, :half], 1)
    far_down = shift(both[2, half:], -1)
    up = shift(jnp.concatenate([both[1, :half] + far_up, both[1, half:]]), 1)
    down = shift(jnp.concatenate([both[3, :half], both[3, half:] + far_down]), -1)
    panel = both[0] + up + down

    slot_index = lax.axis_index("row") * col_count + col_index
    wanted = lax.dynamic_slice_in_dim(kept_vectors, slot_index * every, every)
    source = wanted // block_cols
    earlier = jnp.arange(every, dtype=jnp.int32)
    source_rank = jnp.sum(
        ((source[:, None] == source[None, :]) & (earlier[None, :] < earlier[:, None])).astype(
            jnp.int32
        ),
        axis=1,
    )
    starts = (source * move_cap + source_rank) * lane_tiles
    steps = 4
    per_step = row_count // steps
    in_rows = per_step * col_count * move_cap * lane_tiles
    out_rows = per_step * lane_tiles * SUB
    packed = pl.pallas_call(
        functools.partial(unpack_kernel, lane_tiles, col_count, every, per_step),
        grid=(steps,),
        out_shape=jax.ShapeDtypeStruct((every // SUB, row_count * lane_tiles * SUB, LANES), jnp.float32),
        in_specs=[
            pl.BlockSpec(memory_space=pltpu.SMEM),
            pl.BlockSpec((in_rows, LANES), lambda s: (s, 0)),
        ],
        out_specs=pl.BlockSpec((every // SUB, out_rows, LANES), lambda s: (0, s, 0)),
        name="unpack",
    )(starts, arrived.reshape(dest_count * move_cap * lane_tiles, LANES))
    packed_vectors = from_tiles(packed.reshape(-1, LANES), every, row_count * block_rows)
    return (packed_vectors, panel)


def solution(mesh):
    placed = (P("col", "row"), P(), P(), P(), P(), P(), P())
    return jax.shard_map(
        shards,
        mesh=mesh,
        in_specs=placed,
        out_specs=(P(("row", "col"), None), P("col", "row")),
        check_vma=False,
    )
```

```python
import functools

import jax
import jax.numpy as jnp
from jax import lax
from jax.experimental import pallas as pl
from jax.experimental.pallas import tpu as pltpu
from jax.sharding import PartitionSpec as P


LANES = 128
SUB = 8
GROUP = 8


def tile_view(rows):
    count, width = rows.shape
    tiles = rows.reshape(count // SUB, SUB, width // LANES, LANES).transpose(0, 2, 1, 3)
    return tiles.reshape(count // SUB, width // LANES * SUB, LANES)


def from_tiles(tiles, count, width):
    rows = tiles.reshape(count // SUB, width // LANES, SUB, LANES)
    return rows.transpose(0, 2, 1, 3).reshape(count, width)


def send_kernel(pair_cap, pieces, first_ref, mates_hbm, tiles_hbm, out_hbm,
                mates_ref, tiles_ref, stage_ref, slots_ref, source_ref, sems):
    table = pltpu.make_async_copy(mates_hbm, mates_ref, sems.at[1])
    table.start()
    load = pltpu.make_async_copy(tiles_hbm, tiles_ref, sems.at[0])
    load.start()
    columns, parts = tiles_ref.shape[0] * SUB, stage_ref.shape[1] // SUB
    table.wait()
    count = stage_ref.shape[0]
    blocks = count // pair_cap
    local = columns // LANES
    local_mates = mates_ref[pl.ds(first_ref[0] * local, local), :]
    owner = jnp.concatenate([local_mates[i : i + 1] for i in range(local)], axis=1) // columns
    member = lax.broadcasted_iota(jnp.int32, (blocks, columns), 0) == owner
    earlier = lax.broadcasted_iota(jnp.int32, (columns, columns), 0) < lax.broadcasted_iota(
        jnp.int32, (columns, columns), 1
    )
    before = jnp.dot(
        member.astype(jnp.bfloat16), earlier.astype(jnp.bfloat16),
        preferred_element_type=jnp.float32,
    )
    rank = jnp.sum(jnp.where(member, before, 0.0), axis=0, keepdims=True).astype(jnp.int32)
    place = jnp.where(rank < pair_cap, owner * pair_cap + rank, -1)
    pick = (
        lax.broadcasted_iota(jnp.int32, (count, columns), 0) == place
    ).astype(jnp.bfloat16)
    order = lax.broadcasted_iota(jnp.int32, (SUB, columns), 1)
    digit = lax.broadcasted_iota(jnp.int32, (SUB, columns), 0)
    digits = jnp.where(digit == 0, order // LANES, order % LANES).astype(jnp.bfloat16)
    found = lax.dot_general(
        digits, pick, (((1,), (1,)), ((), ())), preferred_element_type=jnp.float32
    )
    slots_ref[...] = (found[0:1] * LANES + found[1:2]).astype(jnp.int32)
    indices = pltpu.make_async_copy(slots_ref, source_ref, sems.at[1])
    indices.start()
    load.wait()

    indices.wait()

    def group(g, carry):
        values = []
        for n in range(GROUP):
            source = source_ref[0, g * GROUP + n]
            values += [
                tiles_ref[source // SUB, pl.ds(part * SUB * SUB + source % SUB, SUB, SUB), :]
                for part in range(parts)
            ]
        for n, value in enumerate(values):
            stage_ref[g * GROUP + n // parts, pl.ds(n % parts * SUB, SUB), :] = value
        return carry

    piece = count // pieces
    stores = []
    for n in range(pieces):
        lax.fori_loop(n * piece // GROUP, (n + 1) * piece // GROUP, group, 0, unroll=2)
        store = pltpu.make_async_copy(
            stage_ref.at[pl.ds(n * piece, piece)], out_hbm.at[pl.ds(n * piece, piece)], sems.at[2 + n]
        )
        store.start()
        stores.append(store)
    for store in stores:
        store.wait()


def pack_kernel(pieces, source_ref, mate_ref, cos_ref, sin_ref, tiles_hbm, mates_hbm, out_hbm,
                tiles_ref, rows_ref, stage_ref, load_sems, store_sems):
    local_rows, parts = tiles_ref.shape[0] * SUB, rows_ref.shape[1] // SUB
    own_load = pltpu.make_async_copy(tiles_hbm, tiles_ref, load_sems.at[0])
    mate_load = pltpu.make_async_copy(
        mates_hbm, rows_ref.at[pl.ds(local_rows, mates_hbm.shape[0])], load_sems.at[1]
    )
    own_load.start()
    mate_load.start()
    own_load.wait()

    def spread(g, carry):
        values = [
            tiles_ref[g, pl.ds(part * SUB * SUB + s, SUB, SUB), :]
            for s in range(SUB) for part in range(parts)
        ]
        for n, value in enumerate(values):
            rows_ref[g * SUB + n // parts, pl.ds(n % parts * SUB, SUB), :] = value
        return carry

    lax.fori_loop(0, tiles_ref.shape[0], spread, 0, unroll=2)
    mate_load.wait()

    def group(g, carry):
        sources = [source_ref[g * GROUP + n] for n in range(GROUP)]
        values = [cos_ref[i] * rows_ref[i] + sin_ref[i] * rows_ref[mate_ref[i]] for i in sources]
        for n, value in enumerate(values):
            stage_ref[g * GROUP + n] = value
        return carry

    piece = stage_ref.shape[0] // pieces
    stores = []
    for n in range(pieces):
        lax.fori_loop(n * piece // GROUP, (n + 1) * piece // GROUP, group, 0, unroll=2)
        part = pl.ds(n * piece, piece)
        store = pltpu.make_async_copy(stage_ref.at[part], out_hbm.at[part], store_sems.at[n])
        store.start()
        stores.append(store)
    for store in stores:
        store.wait()


def unpack_kernel(wanted, per_step, start_ref, in_ref, out_ref):
    slots = in_ref.shape[0] // per_step
    parts = in_ref.shape[1] // SUB
    for r in range(per_step):
        for first in range(0, wanted, SUB):
            values = [in_ref[start_ref[first + n] + r * slots] for n in range(SUB)]
            for n, value in enumerate(values):
                for part in range(parts):
                    out_ref[first // SUB, r, pl.ds(part * SUB * SUB + n, SUB, SUB), :] = value[
                        part * SUB : (part + 1) * SUB
                    ]


def one_hot_sum(match, values):
    return jnp.sum(jnp.where(match, values[None, :], jnp.zeros((), values.dtype)), axis=1)


def shards(
    eigvec_halves,
    rotation_mate,
    givens_theta,
    kept_vectors,
    secular_singularities,
    secular_coefficients,
    secular_zeros,
):
    col_count = lax.axis_size("col")
    row_count = lax.axis_size("row")
    chips = col_count // 2
    block_cols, block_rows = eigvec_halves.shape
    total_cols = rotation_mate.shape[0]
    panel_cols = secular_zeros.shape[0]
    pair_cap = block_cols // 16
    lane_tiles = block_rows // LANES
    dest_count = row_count * col_count
    every = total_cols // dest_count
    move_cap = every // col_count + every // col_count // 3
    col_index = lax.axis_index("col")
    chip, core = col_index // 2, col_index % 2
    first_col = col_index * block_cols

    order = jnp.arange(block_cols, dtype=jnp.int32)
    labels = first_col + order
    mates = lax.dynamic_slice_in_dim(rotation_mate, first_col, block_cols)
    owner = mates // block_cols
    same_owner = owner[:, None] == owner[None, :]
    tiles = tile_view(eigvec_halves)
    slot_count = col_count * pair_cap
    pieces = 4
    outgoing = pl.pallas_call(
        functools.partial(send_kernel, pair_cap, pieces),
        out_shape=jax.ShapeDtypeStruct((slot_count, lane_tiles, LANES), jnp.float32),
        in_specs=[pl.BlockSpec(memory_space=pltpu.SMEM)] + [pl.BlockSpec(memory_space=pl.ANY)] * 2,
        out_specs=pl.BlockSpec(memory_space=pl.ANY),
        scratch_shapes=[
            pltpu.VMEM((total_cols // LANES, LANES), jnp.int32),
            pltpu.VMEM(tiles.shape, jnp.float32),
            pltpu.VMEM((slot_count, lane_tiles, LANES), jnp.float32),
            pltpu.VMEM((1, slot_count), jnp.int32),
            pltpu.SMEM((1, slot_count), jnp.int32),
            pltpu.SemaphoreType.DMA((2 + pieces,)),
        ],
        name="send",
    )(col_index[None], rotation_mate.reshape(-1, LANES), tiles)
    incoming = lax.all_to_all(outgoing, "col", split_axis=0, concat_axis=0, tiled=True)

    paired = mates != labels
    own_match = kept_vectors[None, :] == labels[:, None]
    mate_match = kept_vectors[None, :] == mates[:, None]
    positions = jnp.arange(total_cols, dtype=jnp.int32)
    spot = one_hot_sum(own_match, positions)
    pole = one_hot_sum(own_match, secular_singularities)
    weight = one_hot_sum(own_match, secular_coefficients)
    mate_pole = one_hot_sum(mate_match, secular_singularities)
    mate_weight = one_hot_sum(mate_match, secular_coefficients)
    angle = one_hot_sum(positions[None, :] == jnp.minimum(labels, mates)[:, None], givens_theta)
    sign_flip = jnp.where(labels < mates, -1.0, 1.0).astype(jnp.float32)
    cosine = jnp.where(paired, jnp.cos(angle), 1.0)
    sine = jnp.where(paired, sign_flip * jnp.sin(angle), 0.0)

    recv_rank = jnp.sum((same_owner & (mates[None, :] < mates[:, None])).astype(jnp.int32), axis=1)
    remote = owner != col_index
    mate_row = jnp.where(remote, block_cols + owner * pair_cap + recv_rank, mates - first_col)
    dest = spot // every
    dest_rank = jnp.sum(
        ((dest[:, None] == dest[None, :]) & (spot[None, :] < spot[:, None])).astype(jnp.int32),
        axis=1,
    )
    dest_slot = dest * move_cap + dest_rank
    places = dest_count * move_cap
    filled = dest_slot[None, :] == jnp.arange(places, dtype=jnp.int32)[:, None]
    place_source = one_hot_sum(filled, order)
    parcels = pl.pallas_call(
        functools.partial(pack_kernel, pieces),
        out_shape=jax.ShapeDtypeStruct((places, lane_tiles, LANES), jnp.float32),
        in_specs=[pl.BlockSpec(memory_space=pltpu.SMEM)] * 4
        + [pl.BlockSpec(memory_space=pl.ANY)] * 2,
        out_specs=pl.BlockSpec(memory_space=pl.ANY),
        scratch_shapes=[
            pltpu.VMEM(tiles.shape, jnp.float32),
            pltpu.VMEM((block_cols + slot_count, lane_tiles, LANES), jnp.float32),
            pltpu.VMEM((places, lane_tiles, LANES), jnp.float32),
            pltpu.SemaphoreType.DMA((2,)),
            pltpu.SemaphoreType.DMA((pieces,)),
        ],
        name="rotate_pack",
    )(place_source, mate_row, cosine, sine, tiles, incoming)
    arrived = lax.all_to_all(
        parcels.reshape(dest_count, move_cap * lane_tiles, LANES),
        ("row", "col"), split_axis=0, concat_axis=0, tiled=True,
    )

    raw = secular_coefficients[:, None] / (secular_singularities[:, None] - secular_zeros[None, :])
    scale_all = lax.rsqrt(jnp.sum(raw * raw, axis=0) + 1e-06)
    by_chip = jnp.stack([secular_zeros, scale_all]).reshape(2, chips, 2, panel_cols // col_count)
    by_chip = jnp.concatenate([by_chip, by_chip], axis=1)
    by_chip = lax.dynamic_slice_in_dim(by_chip, chip, chips, axis=1)

    def partial_panel(parity):
        mine = lax.dynamic_slice_in_dim(by_chip, parity, 1, axis=2).reshape(2, panel_cols // 2)
        zeros, scale = mine[0], mine[1]
        spun = (
            cosine[:, None] * (weight[:, None] / (pole[:, None] - zeros[None, :]))
            - sine[:, None] * (mate_weight[:, None] / (mate_pole[:, None] - zeros[None, :]))
        ) * scale[None, :]
        return lax.dot_general(
            spun, eigvec_halves, (((0,), (0,)), ((), ())),
            precision=lax.Precision.HIGH, preferred_element_type=jnp.float32,
        )

    def shift(array, chip_step):
        pairs = [
            (2 * x + c, 2 * ((x + chip_step) % chips) + c) for x in range(chips) for c in range(2)
        ]
        return lax.ppermute(array, "col", pairs)

    swap = [(c, c ^ 1) for c in range(col_count)]
    theirs = partial_panel(1 - core)
    partner = lax.ppermute(theirs, "col", swap)
    both = (partial_panel(core) + partner).reshape(chips, panel_cols // col_count, block_rows)
    half = panel_cols // col_count // 2
    far_up = shift(both[2, :half], 1)
    far_down = shift(both[2, half:], -1)
    up = shift(jnp.concatenate([both[1, :half] + far_up, both[1, half:]]), 1)
    down = shift(jnp.concatenate([both[3, :half], both[3, half:] + far_down]), -1)

    slot_index = lax.axis_index("row") * col_count + col_index
    wanted = lax.dynamic_slice_in_dim(kept_vectors, slot_index * every, every)
    source = wanted // block_cols
    earlier = jnp.arange(every, dtype=jnp.int32)
    source_rank = jnp.sum(
        ((source[:, None] == source[None, :]) & (earlier[None, :] < earlier[:, None])).astype(
            jnp.int32
        ),
        axis=1,
    )
    starts = source * move_cap + source_rank
    steps = 4
    per_step = row_count // steps
    packed = pl.pallas_call(
        functools.partial(unpack_kernel, every, per_step),
        grid=(steps,),
        out_shape=jax.ShapeDtypeStruct(
            (every // SUB, row_count, lane_tiles * SUB, LANES), jnp.float32
        ),
        in_specs=[
            pl.BlockSpec(memory_space=pltpu.SMEM),
            pl.BlockSpec(
                (per_step * col_count * move_cap, lane_tiles, LANES), lambda s: (s, 0, 0)
            ),
        ],
        out_specs=pl.BlockSpec(
            (every // SUB, per_step, lane_tiles * SUB, LANES), lambda s: (0, s, 0, 0)
        ),
        name="unpack",
    )(starts, arrived.reshape(dest_count * move_cap, lane_tiles, LANES))
    packed_vectors = from_tiles(packed.reshape(-1, LANES), every, row_count * block_rows)
    packed_vectors, up, down = lax.optimization_barrier((packed_vectors, up, down))
    panel = both[0] + up + down
    return (packed_vectors, panel)


def solution(mesh):
    placed = (P("col", "row"), P(), P(), P(), P(), P(), P())

    return jax.shard_map(
        shards,
        mesh=mesh,
        in_specs=placed,
        out_specs=(P(("row", "col"), None), P("col", "row")),
        check_vma=False,
    )
```

```python
import functools

import jax
import jax.numpy as jnp
from jax import lax
from jax.experimental import pallas as pl
from jax.experimental.pallas import tpu as pltpu
from jax.sharding import PartitionSpec as P


LANES = 128
SUB = 8
GROUP = 8


def tile_view(rows):
    count, width = rows.shape
    tiles = rows.reshape(count // SUB, SUB, width // LANES, LANES).transpose(0, 2, 1, 3)
    return tiles.reshape(count // SUB, width // LANES * SUB, LANES)


def from_tiles(tiles, count, width):
    rows = tiles.reshape(count // SUB, width // LANES, SUB, LANES)
    return rows.transpose(0, 2, 1, 3).reshape(count, width)


def send_kernel(pair_cap, pieces, mates_hbm, tiles_hbm, out_hbm,
                mates_ref, tiles_ref, stage_ref, slots_ref, source_ref, sems):
    table = pltpu.make_async_copy(mates_hbm, mates_ref, sems.at[1])
    table.start()
    load = pltpu.make_async_copy(tiles_hbm, tiles_ref, sems.at[0])
    load.start()
    columns, parts = tiles_ref.shape[0] * SUB, stage_ref.shape[1] // SUB
    table.wait()
    count = stage_ref.shape[0]
    blocks = count // pair_cap
    local = columns // LANES
    local_mates = mates_ref[pl.ds(lax.axis_index("col") * local, local), :]
    owner = jnp.concatenate([local_mates[i : i + 1] for i in range(local)], axis=1) // columns
    member = lax.broadcasted_iota(jnp.int32, (blocks, columns), 0) == owner
    earlier = lax.broadcasted_iota(jnp.int32, (columns, columns), 0) < lax.broadcasted_iota(
        jnp.int32, (columns, columns), 1
    )
    before = jnp.dot(
        member.astype(jnp.bfloat16), earlier.astype(jnp.bfloat16),
        preferred_element_type=jnp.float32,
    )
    rank = jnp.sum(jnp.where(member, before, 0.0), axis=0, keepdims=True).astype(jnp.int32)
    place = jnp.where(rank < pair_cap, owner * pair_cap + rank, -1)
    pick = (
        lax.broadcasted_iota(jnp.int32, (count, columns), 0) == place
    ).astype(jnp.bfloat16)
    order = lax.broadcasted_iota(jnp.int32, (SUB, columns), 1)
    digit = lax.broadcasted_iota(jnp.int32, (SUB, columns), 0)
    digits = jnp.where(digit == 0, order // LANES, order % LANES).astype(jnp.bfloat16)
    found = lax.dot_general(
        digits, pick, (((1,), (1,)), ((), ())), preferred_element_type=jnp.float32
    )
    slots_ref[...] = (found[0:1] * LANES + found[1:2]).astype(jnp.int32)
    indices = pltpu.make_async_copy(slots_ref, source_ref, sems.at[1])
    indices.start()
    load.wait()

    indices.wait()

    def group(g, carry):
        values = []
        for n in range(GROUP):
            source = source_ref[0, g * GROUP + n]
            values += [
                tiles_ref[source // SUB, pl.ds(part * SUB * SUB + source % SUB, SUB, SUB), :]
                for part in range(parts)
            ]
        for n, value in enumerate(values):
            stage_ref[g * GROUP + n // parts, pl.ds(n % parts * SUB, SUB), :] = value
        return carry

    piece = count // pieces
    stores = []
    for n in range(pieces):
        lax.fori_loop(n * piece // GROUP, (n + 1) * piece // GROUP, group, 0, unroll=2)
        store = pltpu.make_async_copy(
            stage_ref.at[pl.ds(n * piece, piece)], out_hbm.at[pl.ds(n * piece, piece)], sems.at[2 + n]
        )
        store.start()
        stores.append(store)
    for store in stores:
        store.wait()


def split(value, parts):
    out = []
    for _ in range(parts):
        out.append(value.astype(jnp.bfloat16))
        value = value - out[-1].astype(jnp.float32)
    return out


def panel_kernel(first_ref, mates_ref, theta_ref, kept_ref, pole_ref, weight_ref, zeros_ref, vec_hbm,
                 spot_ref, cos_ref, sin_ref, theirs_hbm, ours_hbm,
                 vec_ref, high_ref, low_ref, wide_high, wide_low, w_high, w_low,
                 theirs_ref, ours_ref, load_sems, store_sems):
    chunks = load_sems.shape[0]
    columns, width = vec_ref.shape
    step = width // chunks
    loads = [
        pltpu.make_async_copy(
            vec_hbm.at[:, pl.ds(n * step, step)], vec_ref.at[:, pl.ds(n * step, step)],
            load_sems.at[n],
        )
        for n in range(chunks)
    ]
    for load in loads:
        load.start()

    total, groups, local = kept_ref.shape[1], mates_ref.shape[0], columns // LANES
    kept = kept_ref[...]
    row_hot = lax.broadcasted_iota(jnp.int32, (groups, total), 0) == kept // LANES
    lane_hot = (
        lax.broadcasted_iota(jnp.int32, (LANES, total), 0) == kept % LANES
    ).astype(jnp.bfloat16)
    place = lax.broadcasted_iota(jnp.int32, (1, total), 1)
    values = [(place // LANES).astype(jnp.float32), (place % LANES).astype(jnp.float32)]
    for ref in (pole_ref, weight_ref):
        values += [part.astype(jnp.float32) for part in split(ref[...], 3)]
    spread = jnp.concatenate([jnp.where(row_hot, value, 0.0) for value in values], axis=0)
    tables = lax.dot_general(
        spread.astype(jnp.bfloat16), lane_hot, (((1,), (1,)), ((), ())),
        preferred_element_type=jnp.float32,
    )
    tables = [tables[n * groups : (n + 1) * groups] for n in range(len(values))]
    tables += [part.astype(jnp.float32) for part in split(theta_ref[...], 3)]

    first = first_ref[0]
    mine = (
        lax.broadcasted_iota(jnp.int32, (groups, LANES), 0) - first * local
    )

    def here(table):
        rows = [
            jnp.sum(jnp.where(mine == n, table, jnp.zeros((), table.dtype)), axis=0, keepdims=True)
            for n in range(local)
        ]
        return jnp.concatenate(rows, axis=1)

    mates = here(mates_ref[...])
    labels = first * columns + lax.broadcasted_iota(jnp.int32, (1, columns), 1)
    mate_lane = (
        lax.broadcasted_iota(jnp.int32, (LANES, columns), 0) == mates % LANES
    ).astype(jnp.bfloat16)
    mate_row = lax.broadcasted_iota(jnp.int32, (groups, columns), 0) == mates // LANES
    wanted = jnp.concatenate(tables[2:], axis=0).astype(jnp.bfloat16)
    picked = jnp.dot(wanted, mate_lane, preferred_element_type=jnp.float32)
    theirs = [
        jnp.sum(
            jnp.where(mate_row, picked[n * groups : (n + 1) * groups], 0.0), axis=0, keepdims=True
        )
        for n in range(9)
    ]
    mate_pole, mate_weight, mate_theta = [
        theirs[n] + (theirs[n + 1] + theirs[n + 2]) for n in (0, 3, 6)
    ]
    spot_ref[...] = here(tables[0] * LANES + tables[1]).astype(jnp.int32)
    pole = here(tables[2] + (tables[3] + tables[4]))
    weight = here(tables[5] + (tables[6] + tables[7]))
    angle = jnp.where(mates < labels, mate_theta, here(theta_ref[...]))
    paired = mates != labels
    cosine = jnp.where(paired, jnp.cos(angle), 1.0)
    sine = jnp.where(paired, jnp.where(labels < mates, -1.0, 1.0) * jnp.sin(angle), 0.0)
    cos_ref[...] = cosine
    sin_ref[...] = sine

    own_part, mate_part = cosine * weight, sine * mate_weight
    for q in range(zeros_ref.shape[0]):
        zeros = jnp.broadcast_to(zeros_ref[q : q + 1], (LANES, LANES)).T
        for t in range(local):
            at = slice(t * LANES, (t + 1) * LANES)
            value = own_part[:, at] / (pole[:, at] - zeros) - mate_part[:, at] / (
                mate_pole[:, at] - zeros
            )
            high, low = split(value, 2)
            wide_high[q * LANES : (q + 1) * LANES, at] = high
            wide_low[q * LANES : (q + 1) * LANES, at] = low

    half = theirs_ref.shape[0]
    block = half // 4
    chip, core = first // 2, first % 2
    count = half // block
    for parity in range(2):
        for distance in range(count):
            owner = (chip + distance) % count * 2 + (1 - core if parity == 0 else core)
            source = pl.ds(pl.multiple_of(owner * block, block), block)
            target = slice(parity * half + distance * block, parity * half + (distance + 1) * block)
            w_high[target, :] = wide_high[source, :]
            w_low[target, :] = wide_low[source, :]

    stores = []
    for parity, (stage, out) in enumerate(((theirs_ref, theirs_hbm), (ours_ref, ours_hbm))):
        rows = slice(parity * half, (parity + 1) * half)
        for n in range(chunks):
            at = slice(n * step, (n + 1) * step)
            if parity == 0:
                loads[n].wait()
                high_ref[:, at], low_ref[:, at] = split(vec_ref[:, at], 2)
            high, low = high_ref[:, at], low_ref[:, at]
            stage[:, at] = (
                jnp.dot(w_high[rows, :], high, preferred_element_type=jnp.float32)
                + jnp.dot(w_high[rows, :], low, preferred_element_type=jnp.float32)
                + jnp.dot(w_low[rows, :], high, preferred_element_type=jnp.float32)
            )
            part = pl.ds(n * step, step)
            store = pltpu.make_async_copy(
                stage.at[:, part], out.at[:, part], store_sems.at[parity * chunks + n]
            )
            store.start()
            stores.append(store)
    for store in stores:
        store.wait()


def pack_kernel(pieces, source_hbm, mate_hbm, cos_hbm, sin_hbm, tiles_hbm, mates_hbm, out_hbm,
                source_ref, mate_ref, cos_ref, sin_ref, tiles_ref, rows_ref, stage_ref,
                load_sems, store_sems):
    local_rows, parts = tiles_ref.shape[0] * SUB, rows_ref.shape[1] // SUB
    own_load = pltpu.make_async_copy(tiles_hbm, tiles_ref, load_sems.at[0])
    mate_load = pltpu.make_async_copy(
        mates_hbm, rows_ref.at[pl.ds(local_rows, mates_hbm.shape[0])], load_sems.at[1]
    )
    own_load.start()
    mate_load.start()
    tables = [
        pltpu.make_async_copy(table, ref, load_sems.at[2 + n])
        for n, (table, ref) in enumerate((
            (source_hbm, source_ref), (mate_hbm, mate_ref), (cos_hbm, cos_ref), (sin_hbm, sin_ref)
        ))
    ]
    for table in tables:
        table.start()
    own_load.wait()

    def spread(g, carry):
        values = [
            tiles_ref[g, pl.ds(part * SUB * SUB + s, SUB, SUB), :]
            for s in range(SUB) for part in range(parts)
        ]
        for n, value in enumerate(values):
            rows_ref[g * SUB + n // parts, pl.ds(n % parts * SUB, SUB), :] = value
        return carry

    lax.fori_loop(0, tiles_ref.shape[0], spread, 0, unroll=2)
    for table in tables:
        table.wait()
    mate_load.wait()

    def group(g, carry):
        sources = [source_ref[0, g * GROUP + n] for n in range(GROUP)]
        values = [
            cos_ref[0, i] * rows_ref[i] + sin_ref[0, i] * rows_ref[mate_ref[0, i]] for i in sources
        ]
        for n, value in enumerate(values):
            stage_ref[g * GROUP + n] = value
        return carry

    piece = stage_ref.shape[0] // pieces
    stores = []
    for n in range(pieces):
        lax.fori_loop(n * piece // GROUP, (n + 1) * piece // GROUP, group, 0, unroll=2)
        part = pl.ds(n * piece, piece)
        store = pltpu.make_async_copy(stage_ref.at[part], out_hbm.at[part], store_sems.at[n])
        store.start()
        stores.append(store)
    for store in stores:
        store.wait()


def unpack_kernel(start_hbm, in_hbm, out_hbm, start_ref, in_ref, out_ref,
                  table_sem, load_sems, store_sems):
    pieces = load_sems.shape[0]
    rows, parts = in_ref.shape[0], in_ref.shape[2] // SUB
    wanted, per = start_ref.shape[1], rows // pieces
    table = pltpu.make_async_copy(start_hbm, start_ref, table_sem)
    table.start()
    loads, stores = [], []
    for n in range(pieces):
        part = pl.ds(n * per, per)
        loads.append(pltpu.make_async_copy(in_hbm.at[part], in_ref.at[part], load_sems.at[n]))
        stores.append(
            pltpu.make_async_copy(out_ref.at[:, part], out_hbm.at[:, part], store_sems.at[n])
        )
        loads[n].start()
    table.wait()
    for n in range(pieces):
        loads[n].wait()

        def row(r, carry):
            for first in range(0, wanted, SUB):
                values = [in_ref[r, start_ref[0, first + k]] for k in range(SUB)]
                for k, value in enumerate(values):
                    for part in range(parts):
                        out_ref[first // SUB, r, pl.ds(part * SUB * SUB + k, SUB, SUB), :] = value[
                            part * SUB : (part + 1) * SUB
                        ]
            return carry

        lax.fori_loop(n * per, (n + 1) * per, row, 0)
        stores[n].start()
    for store in stores:
        store.wait()


def one_hot_sum(match, values):
    return jnp.sum(jnp.where(match, values[None, :], jnp.zeros((), values.dtype)), axis=1)


def shards(
    eigvec_halves,
    rotation_mate,
    givens_theta,
    kept_vectors,
    secular_singularities,
    secular_coefficients,
    secular_zeros,
):
    col_count = lax.axis_size("col")
    row_count = lax.axis_size("row")
    chips = col_count // 2
    block_cols, block_rows = eigvec_halves.shape
    total_cols = rotation_mate.shape[0]
    panel_cols = secular_zeros.shape[0]
    pair_cap = block_cols // 16
    lane_tiles = block_rows // LANES
    dest_count = row_count * col_count
    every = total_cols // dest_count
    move_cap = every // col_count + every // col_count // 3
    col_index = lax.axis_index("col")
    first_col = col_index * block_cols

    order = jnp.arange(block_cols, dtype=jnp.int32)
    mates = lax.dynamic_slice_in_dim(rotation_mate, first_col, block_cols)
    owner = mates // block_cols
    same_owner = owner[:, None] == owner[None, :]
    tiles = tile_view(eigvec_halves)
    slot_count = col_count * pair_cap
    pieces = 4
    outgoing = pl.pallas_call(
        functools.partial(send_kernel, pair_cap, pieces),
        out_shape=jax.ShapeDtypeStruct((slot_count, lane_tiles, LANES), jnp.float32),
        in_specs=[pl.BlockSpec(memory_space=pl.ANY)] * 2,
        out_specs=pl.BlockSpec(memory_space=pl.ANY),
        scratch_shapes=[
            pltpu.VMEM((total_cols // LANES, LANES), jnp.int32),
            pltpu.VMEM(tiles.shape, jnp.float32),
            pltpu.VMEM((slot_count, lane_tiles, LANES), jnp.float32),
            pltpu.VMEM((1, slot_count), jnp.int32),
            pltpu.SMEM((1, slot_count), jnp.int32),
            pltpu.SemaphoreType.DMA((2 + pieces,)),
        ],
        name="send",
    )(rotation_mate.reshape(-1, LANES), tiles)
    incoming = lax.all_to_all(outgoing, "col", split_axis=0, concat_axis=0, tiled=True)

    half_cols = panel_cols // 2
    vec_chunks = 4
    spot, cosine, sine, theirs, ours = pl.pallas_call(
        panel_kernel,
        out_shape=[
            jax.ShapeDtypeStruct((1, block_cols), jnp.int32),
            jax.ShapeDtypeStruct((1, block_cols), jnp.float32),
            jax.ShapeDtypeStruct((1, block_cols), jnp.float32),
            jax.ShapeDtypeStruct((half_cols, block_rows), jnp.float32),
            jax.ShapeDtypeStruct((half_cols, block_rows), jnp.float32),
        ],
        in_specs=[pl.BlockSpec(memory_space=pltpu.SMEM)]
        + [pl.BlockSpec(memory_space=pltpu.VMEM)] * 6
        + [pl.BlockSpec(memory_space=pl.ANY)],
        out_specs=[pl.BlockSpec(memory_space=pltpu.VMEM)] * 3
        + [pl.BlockSpec(memory_space=pl.ANY)] * 2,
        scratch_shapes=[
            pltpu.VMEM((block_cols, block_rows), jnp.float32),
            pltpu.VMEM((block_cols, block_rows), jnp.bfloat16),
            pltpu.VMEM((block_cols, block_rows), jnp.bfloat16),
            pltpu.VMEM((panel_cols, block_cols), jnp.bfloat16),
            pltpu.VMEM((panel_cols, block_cols), jnp.bfloat16),
            pltpu.VMEM((panel_cols, block_cols), jnp.bfloat16),
            pltpu.VMEM((panel_cols, block_cols), jnp.bfloat16),
            pltpu.VMEM((half_cols, block_rows), jnp.float32),
            pltpu.VMEM((half_cols, block_rows), jnp.float32),
            pltpu.SemaphoreType.DMA((vec_chunks,)),
            pltpu.SemaphoreType.DMA((2 * vec_chunks,)),
        ],
        name="panel",
    )(
        col_index[None],
        rotation_mate.reshape(-1, LANES),
        givens_theta.reshape(-1, LANES),
        kept_vectors[None, :],
        secular_singularities[None, :],
        secular_coefficients[None, :],
        secular_zeros.reshape(-1, LANES),
        eigvec_halves,
    )
    spot = spot[0]
    recv_rank = jnp.sum((same_owner & (mates[None, :] < mates[:, None])).astype(jnp.int32), axis=1)
    remote = owner != col_index
    mate_row = jnp.where(remote, block_cols + owner * pair_cap + recv_rank, mates - first_col)
    dest = spot // every
    dest_rank = jnp.sum(
        ((dest[:, None] == dest[None, :]) & (spot[None, :] < spot[:, None])).astype(jnp.int32),
        axis=1,
    )
    dest_slot = dest * move_cap + dest_rank
    places = dest_count * move_cap
    filled = dest_slot[None, :] == jnp.arange(places, dtype=jnp.int32)[:, None]
    place_source = one_hot_sum(filled, order)
    parcels = pl.pallas_call(
        functools.partial(pack_kernel, pieces),
        out_shape=jax.ShapeDtypeStruct((places, lane_tiles, LANES), jnp.float32),
        in_specs=[pl.BlockSpec(memory_space=pl.ANY)] * 6,
        out_specs=pl.BlockSpec(memory_space=pl.ANY),
        scratch_shapes=[
            pltpu.SMEM((1, places), jnp.int32),
            pltpu.SMEM((1, block_cols), jnp.int32),
            pltpu.SMEM((1, block_cols), jnp.float32),
            pltpu.SMEM((1, block_cols), jnp.float32),
            pltpu.VMEM(tiles.shape, jnp.float32),
            pltpu.VMEM((block_cols + slot_count, lane_tiles, LANES), jnp.float32),
            pltpu.VMEM((places, lane_tiles, LANES), jnp.float32),
            pltpu.SemaphoreType.DMA((6,)),
            pltpu.SemaphoreType.DMA((pieces,)),
        ],
        compiler_params=pltpu.CompilerParams(vmem_limit_bytes=50 * 1024 * 1024),
        name="rotate_pack",
    )(place_source[None, :], mate_row[None, :], cosine, sine, tiles, incoming)
    arrived = lax.all_to_all(
        parcels.reshape(dest_count, move_cap * lane_tiles, LANES),
        ("row", "col"), split_axis=0, concat_axis=0, tiled=True,
    )

    share = panel_cols // col_count
    zeros_here = lax.dynamic_slice_in_dim(secular_zeros, col_index * share, share)
    raw = secular_coefficients[:, None] / (secular_singularities[:, None] - zeros_here[None, :])
    scale = lax.rsqrt(jnp.sum(raw * raw, axis=0) + 1e-06)

    def shift(array, chip_step):
        pairs = [
            (2 * x + c, 2 * ((x + chip_step) % chips) + c) for x in range(chips) for c in range(2)
        ]
        return lax.ppermute(array, "col", pairs)

    swap = [(c, c ^ 1) for c in range(col_count)]
    partner = lax.ppermute(theirs, "col", swap)
    ours = ours.reshape(chips, share, block_rows)
    partner = partner.reshape(chips, share, block_rows)
    half = share // 2

    def pair(distance, rows):
        return ours[distance, rows] + partner[distance, rows]

    low, high = slice(0, half), slice(half, share)
    up = shift(jnp.concatenate([pair(2, low), pair(1, high)]), 1)
    down = shift(jnp.concatenate([pair(2, high), pair(3, low)]), -1)
    up_low = shift(pair(1, low) + up[:half], 1)
    down_high = shift(pair(3, high) + down[:half], -1)

    slot_index = lax.axis_index("row") * col_count + col_index
    wanted = lax.dynamic_slice_in_dim(kept_vectors, slot_index * every, every)
    source = wanted // block_cols
    earlier = jnp.arange(every, dtype=jnp.int32)
    source_rank = jnp.sum(
        ((source[:, None] == source[None, :]) & (earlier[None, :] < earlier[:, None])).astype(
            jnp.int32
        ),
        axis=1,
    )
    starts = source * move_cap + source_rank
    packed = pl.pallas_call(
        unpack_kernel,
        out_shape=jax.ShapeDtypeStruct(
            (every // SUB, row_count, lane_tiles * SUB, LANES), jnp.float32
        ),
        in_specs=[pl.BlockSpec(memory_space=pl.ANY)] * 2,
        out_specs=pl.BlockSpec(memory_space=pl.ANY),
        scratch_shapes=[
            pltpu.SMEM((1, every), jnp.int32),
            pltpu.VMEM((row_count, col_count * move_cap, lane_tiles, LANES), jnp.float32),
            pltpu.VMEM((every // SUB, row_count, lane_tiles * SUB, LANES), jnp.float32),
            pltpu.SemaphoreType.DMA,
            pltpu.SemaphoreType.DMA((pieces,)),
            pltpu.SemaphoreType.DMA((pieces,)),
        ],
        name="unpack",
    )(starts[None, :], arrived.reshape(row_count, col_count * move_cap, lane_tiles, LANES))
    packed_vectors = from_tiles(packed.reshape(-1, LANES), every, row_count * block_rows)
    base = pair(0, slice(0, share)) + jnp.concatenate([down[half:], up[half:]])
    base = lax.optimization_barrier(base * scale[:, None])
    packed_vectors, up_low, down_high = lax.optimization_barrier((packed_vectors, up_low, down_high))
    panel = base + jnp.concatenate([up_low, down_high]) * scale[:, None]
    return (packed_vectors, panel)


def solution(mesh):
    placed = (P("col", "row"), P(), P(), P(), P(), P(), P())

    return jax.shard_map(
        shards,
        mesh=mesh,
        in_specs=placed,
        out_specs=(P(("row", "col"), None), P("col", "row")),
        check_vma=False,
    )
```

```python
import functools

import jax
import jax.numpy as jnp
from jax import lax
from jax.experimental import pallas as pl
from jax.experimental.pallas import tpu as pltpu
from jax.sharding import PartitionSpec as P


LANES = 128
SUB = 8
GROUP = 8


def tile_view(rows):
    count, width = rows.shape
    tiles = rows.reshape(count // SUB, SUB, width // LANES, LANES).transpose(0, 2, 1, 3)
    return tiles.reshape(count // SUB, width // LANES * SUB, LANES)


def from_tiles(tiles, count, width):
    rows = tiles.reshape(count // SUB, width // LANES, SUB, LANES)
    return rows.transpose(0, 2, 1, 3).reshape(count, width)


def send_kernel(pair_cap, pieces, mates_hbm, tiles_hbm, out_hbm,
                mates_ref, tiles_ref, stage_ref, slots_ref, source_ref, sems):
    table = pltpu.make_async_copy(mates_hbm, mates_ref, sems.at[1])
    table.start()
    load = pltpu.make_async_copy(tiles_hbm, tiles_ref, sems.at[0])
    load.start()
    columns, parts = tiles_ref.shape[0] * SUB, stage_ref.shape[1] // SUB
    table.wait()
    count = stage_ref.shape[0]
    blocks = count // pair_cap
    local = columns // LANES
    local_mates = mates_ref[pl.ds(lax.axis_index("col") * local, local), :]
    owner = jnp.concatenate([local_mates[i : i + 1] for i in range(local)], axis=1) // columns
    member = lax.broadcasted_iota(jnp.int32, (blocks, columns), 0) == owner
    earlier = lax.broadcasted_iota(jnp.int32, (columns, columns), 0) < lax.broadcasted_iota(
        jnp.int32, (columns, columns), 1
    )
    before = jnp.dot(
        member.astype(jnp.bfloat16), earlier.astype(jnp.bfloat16),
        preferred_element_type=jnp.float32,
    )
    rank = jnp.sum(jnp.where(member, before, 0.0), axis=0, keepdims=True).astype(jnp.int32)
    place = jnp.where(rank < pair_cap, owner * pair_cap + rank, -1)
    pick = (
        lax.broadcasted_iota(jnp.int32, (count, columns), 0) == place
    ).astype(jnp.bfloat16)
    order = lax.broadcasted_iota(jnp.int32, (SUB, columns), 1)
    digit = lax.broadcasted_iota(jnp.int32, (SUB, columns), 0)
    digits = jnp.where(digit == 0, order // LANES, order % LANES).astype(jnp.bfloat16)
    found = lax.dot_general(
        digits, pick, (((1,), (1,)), ((), ())), preferred_element_type=jnp.float32
    )
    slots_ref[...] = (found[0:1] * LANES + found[1:2]).astype(jnp.int32)
    indices = pltpu.make_async_copy(slots_ref, source_ref, sems.at[1])
    indices.start()
    load.wait()

    indices.wait()

    def group(g, carry):
        values = []
        for n in range(GROUP):
            source = source_ref[0, g * GROUP + n]
            values += [
                tiles_ref[source // SUB, pl.ds(part * SUB * SUB + source % SUB, SUB, SUB), :]
                for part in range(parts)
            ]
        for n, value in enumerate(values):
            stage_ref[g * GROUP + n // parts, pl.ds(n % parts * SUB, SUB), :] = value
        return carry

    piece = count // pieces
    stores = []
    for n in range(pieces):
        lax.fori_loop(n * piece // GROUP, (n + 1) * piece // GROUP, group, 0, unroll=2)
        store = pltpu.make_async_copy(
            stage_ref.at[pl.ds(n * piece, piece)], out_hbm.at[pl.ds(n * piece, piece)], sems.at[2 + n]
        )
        store.start()
        stores.append(store)
    for store in stores:
        store.wait()


def split(value, parts):
    out = []
    for _ in range(parts):
        out.append(value.astype(jnp.bfloat16))
        value = value - out[-1].astype(jnp.float32)
    return out


def panel_kernel(mates_ref, theta_ref, kept_ref, pole_ref, weight_ref, zeros_ref, vec_hbm,
                 spot_ref, cos_ref, sin_ref, theirs_hbm, ours_hbm,
                 vec_ref, deep_ref, wide_high, wide_low, w_ref,
                 theirs_ref, ours_ref, load_sems, store_sems):
    chunks = load_sems.shape[0]
    columns, width = vec_ref.shape
    step = width // chunks
    loads = [
        pltpu.make_async_copy(
            vec_hbm.at[:, pl.ds(n * step, step)], vec_ref.at[:, pl.ds(n * step, step)],
            load_sems.at[n],
        )
        for n in range(chunks)
    ]
    for load in loads:
        load.start()

    total, groups, local = kept_ref.shape[1], mates_ref.shape[0], columns // LANES
    kept = kept_ref[...]
    row_hot = lax.broadcasted_iota(jnp.int32, (groups, total), 0) == kept // LANES
    lane_hot = (
        lax.broadcasted_iota(jnp.int32, (LANES, total), 0) == kept % LANES
    ).astype(jnp.bfloat16)
    place = lax.broadcasted_iota(jnp.int32, (1, total), 1)
    values = [(place // LANES).astype(jnp.float32), (place % LANES).astype(jnp.float32)]
    for ref in (pole_ref, weight_ref):
        values += [part.astype(jnp.float32) for part in split(ref[...], 3)]
    spread = jnp.concatenate([jnp.where(row_hot, value, 0.0) for value in values], axis=0)
    tables = lax.dot_general(
        spread.astype(jnp.bfloat16), lane_hot, (((1,), (1,)), ((), ())),
        preferred_element_type=jnp.float32,
    )
    tables = [tables[n * groups : (n + 1) * groups] for n in range(len(values))]
    tables += [part.astype(jnp.float32) for part in split(theta_ref[...], 3)]

    first = lax.axis_index("col")
    mine = (
        lax.broadcasted_iota(jnp.int32, (groups, LANES), 0) - first * local
    )

    def here(table):
        rows = [
            jnp.sum(jnp.where(mine == n, table, jnp.zeros((), table.dtype)), axis=0, keepdims=True)
            for n in range(local)
        ]
        return jnp.concatenate(rows, axis=1)

    mates = here(mates_ref[...])
    labels = first * columns + lax.broadcasted_iota(jnp.int32, (1, columns), 1)
    mate_lane = (
        lax.broadcasted_iota(jnp.int32, (LANES, columns), 0) == mates % LANES
    ).astype(jnp.bfloat16)
    mate_row = lax.broadcasted_iota(jnp.int32, (groups, columns), 0) == mates // LANES
    wanted = jnp.concatenate(tables[2:], axis=0).astype(jnp.bfloat16)
    picked = jnp.dot(wanted, mate_lane, preferred_element_type=jnp.float32)
    theirs = [
        jnp.sum(
            jnp.where(mate_row, picked[n * groups : (n + 1) * groups], 0.0), axis=0, keepdims=True
        )
        for n in range(9)
    ]
    mate_pole, mate_weight, mate_theta = [
        theirs[n] + (theirs[n + 1] + theirs[n + 2]) for n in (0, 3, 6)
    ]
    spot_ref[...] = here(tables[0] * LANES + tables[1]).astype(jnp.int32)
    pole = here(tables[2] + (tables[3] + tables[4]))
    weight = here(tables[5] + (tables[6] + tables[7]))
    angle = jnp.where(mates < labels, mate_theta, here(theta_ref[...]))
    paired = mates != labels
    cosine = jnp.where(paired, jnp.cos(angle), 1.0)
    sine = jnp.where(paired, jnp.where(labels < mates, -1.0, 1.0) * jnp.sin(angle), 0.0)
    cos_ref[...] = cosine
    sin_ref[...] = sine

    own_part, mate_part = cosine * weight, sine * mate_weight
    for q in range(zeros_ref.shape[0]):
        zeros = jnp.broadcast_to(zeros_ref[q : q + 1], (LANES, LANES)).T
        for t in range(local):
            at = slice(t * LANES, (t + 1) * LANES)
            value = own_part[:, at] / (pole[:, at] - zeros) - mate_part[:, at] / (
                mate_pole[:, at] - zeros
            )
            high, low = split(value, 2)
            wide_high[q * LANES : (q + 1) * LANES, at] = high
            wide_low[q * LANES : (q + 1) * LANES, at] = low

    half = theirs_ref.shape[0]
    block = half // 4
    chip, core = first // 2, first % 2
    count = half // block
    for parity in range(2):
        for distance in range(count):
            owner = (chip + distance) % count * 2 + (1 - core if parity == 0 else core)
            source = pl.ds(pl.multiple_of(owner * block, block), block)
            target = slice(parity * half + distance * block, parity * half + (distance + 1) * block)
            w_ref[target, 0:columns] = wide_high[source, :]
            w_ref[target, columns : 2 * columns] = wide_high[source, :]
            w_ref[target, 2 * columns :] = wide_low[source, :]

    stores = []
    for parity, (stage, out) in enumerate(((theirs_ref, theirs_hbm), (ours_ref, ours_hbm))):
        rows = slice(parity * half, (parity + 1) * half)
        for n in range(chunks):
            at = slice(n * step, (n + 1) * step)
            if parity == 0:
                loads[n].wait()
                high, low = split(vec_ref[:, at], 2)
                deep_ref[0:columns, at] = high
                deep_ref[columns : 2 * columns, at] = low
                deep_ref[2 * columns :, at] = high
            stage[:, at] = jnp.dot(
                w_ref[rows, :], deep_ref[:, at], preferred_element_type=jnp.float32
            )
            part = pl.ds(n * step, step)
            store = pltpu.make_async_copy(
                stage.at[:, part], out.at[:, part], store_sems.at[parity * chunks + n]
            )
            store.start()
            stores.append(store)
    for store in stores:
        store.wait()


def turn_kernel(mate_hbm, cos_hbm, sin_hbm, tiles_hbm, turned_ref,
                mate_ref, cos_ref, sin_ref, tiles_ref, rows_ref, sems):
    loads = [
        pltpu.make_async_copy(source, ref, sems.at[n])
        for n, (source, ref) in enumerate((
            (tiles_hbm, tiles_ref), (mate_hbm, mate_ref), (cos_hbm, cos_ref), (sin_hbm, sin_ref)
        ))
    ]
    for load in loads:
        load.start()
    loads[0].wait()
    parts = rows_ref.shape[1] // SUB

    def spread(g, carry):
        values = [
            tiles_ref[g, pl.ds(part * SUB * SUB + s, SUB, SUB), :]
            for s in range(SUB) for part in range(parts)
        ]
        for n, value in enumerate(values):
            rows_ref[g * SUB + n // parts, pl.ds(n % parts * SUB, SUB), :] = value
        return carry

    lax.fori_loop(0, tiles_ref.shape[0], spread, 0, unroll=2)
    for load in loads[1:]:
        load.wait()

    def turn(g, carry):
        columns = [g * GROUP + n for n in range(GROUP)]
        values = [
            cos_ref[0, i] * rows_ref[i] + sin_ref[0, i] * rows_ref[mate_ref[0, i]] for i in columns
        ]
        for i, value in zip(columns, values):
            turned_ref[i] = value
        return carry

    lax.fori_loop(0, rows_ref.shape[0] // GROUP, turn, 0, unroll=2)


def pack_kernel(pieces, source_hbm, mate_hbm, sin_hbm, turned_ref, mates_ref, out_hbm,
                source_ref, mate_ref, sin_ref, stage_ref, load_sems, store_sems):
    tables = [
        pltpu.make_async_copy(table, ref, load_sems.at[n])
        for n, (table, ref) in enumerate(
            ((source_hbm, source_ref), (mate_hbm, mate_ref), (sin_hbm, sin_ref))
        )
    ]
    for table in tables:
        table.start()
    for table in tables:
        table.wait()

    def group(g, carry):
        sources = [source_ref[0, g * GROUP + n] for n in range(GROUP)]
        values = [turned_ref[i] + sin_ref[0, i] * mates_ref[mate_ref[0, i]] for i in sources]
        for n, value in enumerate(values):
            stage_ref[g * GROUP + n] = value
        return carry

    piece = stage_ref.shape[0] // pieces
    stores = []
    for n in range(pieces):
        lax.fori_loop(n * piece // GROUP, (n + 1) * piece // GROUP, group, 0, unroll=2)
        part = pl.ds(n * piece, piece)
        store = pltpu.make_async_copy(stage_ref.at[part], out_hbm.at[part], store_sems.at[n])
        store.start()
        stores.append(store)
    for store in stores:
        store.wait()


def unpack_kernel(start_hbm, in_hbm, out_hbm, start_ref, in_ref, out_ref,
                  table_sem, load_sems, store_sems):
    pieces = load_sems.shape[0]
    rows, parts = in_ref.shape[0], in_ref.shape[2] // SUB
    wanted, per = start_ref.shape[1], rows // pieces
    table = pltpu.make_async_copy(start_hbm, start_ref, table_sem)
    table.start()
    loads, stores = [], []
    for n in range(pieces):
        part = pl.ds(n * per, per)
        loads.append(pltpu.make_async_copy(in_hbm.at[part], in_ref.at[part], load_sems.at[n]))
        stores.append(
            pltpu.make_async_copy(out_ref.at[:, part], out_hbm.at[:, part], store_sems.at[n])
        )
        loads[n].start()
    table.wait()
    for n in range(pieces):
        loads[n].wait()

        def row(r, carry):
            for first in range(0, wanted, SUB):
                values = [in_ref[r, start_ref[0, first + k]] for k in range(SUB)]
                for k, value in enumerate(values):
                    for part in range(parts):
                        out_ref[first // SUB, r, pl.ds(part * SUB * SUB + k, SUB, SUB), :] = value[
                            part * SUB : (part + 1) * SUB
                        ]
            return carry

        lax.fori_loop(n * per, (n + 1) * per, row, 0)
        stores[n].start()
    for store in stores:
        store.wait()


def one_hot_sum(match, values):
    return jnp.sum(jnp.where(match, values[None, :], jnp.zeros((), values.dtype)), axis=1)


def shards(
    eigvec_halves,
    rotation_mate,
    givens_theta,
    kept_vectors,
    secular_singularities,
    secular_coefficients,
    secular_zeros,
):
    col_count = lax.axis_size("col")
    row_count = lax.axis_size("row")
    chips = col_count // 2
    block_cols, block_rows = eigvec_halves.shape
    total_cols = rotation_mate.shape[0]
    panel_cols = secular_zeros.shape[0]
    pair_cap = block_cols // 16
    lane_tiles = block_rows // LANES
    dest_count = row_count * col_count
    every = total_cols // dest_count
    move_cap = every // col_count + every // col_count // 3
    col_index = lax.axis_index("col")
    first_col = col_index * block_cols

    order = jnp.arange(block_cols, dtype=jnp.int32)
    mates = lax.dynamic_slice_in_dim(rotation_mate, first_col, block_cols)
    owner = mates // block_cols
    same_owner = owner[:, None] == owner[None, :]
    tiles = tile_view(eigvec_halves)
    slot_count = col_count * pair_cap
    pieces = 4
    outgoing = pl.pallas_call(
        functools.partial(send_kernel, pair_cap, pieces),
        out_shape=jax.ShapeDtypeStruct((slot_count, lane_tiles, LANES), jnp.float32),
        in_specs=[pl.BlockSpec(memory_space=pl.ANY)] * 2,
        out_specs=pl.BlockSpec(memory_space=pl.ANY),
        scratch_shapes=[
            pltpu.VMEM((total_cols // LANES, LANES), jnp.int32),
            pltpu.VMEM(tiles.shape, jnp.float32),
            pltpu.VMEM((slot_count, lane_tiles, LANES), jnp.float32),
            pltpu.VMEM((1, slot_count), jnp.int32),
            pltpu.SMEM((1, slot_count), jnp.int32),
            pltpu.SemaphoreType.DMA((2 + pieces,)),
        ],
        name="send",
    )(rotation_mate.reshape(-1, LANES), tiles)
    incoming = lax.all_to_all(outgoing, "col", split_axis=0, concat_axis=0, tiled=True)

    half_cols = panel_cols // 2
    vec_chunks = 2
    spot, cosine, sine, theirs, ours = pl.pallas_call(
        panel_kernel,
        out_shape=[
            jax.ShapeDtypeStruct((1, block_cols), jnp.int32),
            jax.ShapeDtypeStruct((1, block_cols), jnp.float32),
            jax.ShapeDtypeStruct((1, block_cols), jnp.float32),
            jax.ShapeDtypeStruct((half_cols, block_rows), jnp.float32),
            jax.ShapeDtypeStruct((half_cols, block_rows), jnp.float32),
        ],
        in_specs=[pl.BlockSpec(memory_space=pltpu.VMEM)] * 6
        + [pl.BlockSpec(memory_space=pl.ANY)],
        out_specs=[pl.BlockSpec(memory_space=pltpu.VMEM)] * 3
        + [pl.BlockSpec(memory_space=pl.ANY)] * 2,
        scratch_shapes=[
            pltpu.VMEM((block_cols, block_rows), jnp.float32),
            pltpu.VMEM((3 * block_cols, block_rows), jnp.bfloat16),
            pltpu.VMEM((panel_cols, block_cols), jnp.bfloat16),
            pltpu.VMEM((panel_cols, block_cols), jnp.bfloat16),
            pltpu.VMEM((panel_cols, 3 * block_cols), jnp.bfloat16),
            pltpu.VMEM((half_cols, block_rows), jnp.float32),
            pltpu.VMEM((half_cols, block_rows), jnp.float32),
            pltpu.SemaphoreType.DMA((vec_chunks,)),
            pltpu.SemaphoreType.DMA((2 * vec_chunks,)),
        ],
        name="panel",
    )(
        rotation_mate.reshape(-1, LANES),
        givens_theta.reshape(-1, LANES),
        kept_vectors[None, :],
        secular_singularities[None, :],
        secular_coefficients[None, :],
        secular_zeros.reshape(-1, LANES),
        eigvec_halves,
    )
    spot = spot[0]
    recv_rank = jnp.sum((same_owner & (mates[None, :] < mates[:, None])).astype(jnp.int32), axis=1)
    remote = owner != col_index
    mate_row = jnp.where(remote, owner * pair_cap + recv_rank, 0)
    far_sine = jnp.where(remote[None, :], sine, 0.0)
    turned = pl.pallas_call(
        turn_kernel,
        out_shape=pltpu.VMEM((block_cols, lane_tiles, LANES), jnp.float32),
        in_specs=[pl.BlockSpec(memory_space=pl.ANY)] * 4,
        out_specs=pl.BlockSpec(memory_space=pltpu.VMEM),
        scratch_shapes=[
            pltpu.SMEM((1, block_cols), jnp.int32),
            pltpu.SMEM((1, block_cols), jnp.float32),
            pltpu.SMEM((1, block_cols), jnp.float32),
            pltpu.VMEM(tiles.shape, jnp.float32),
            pltpu.VMEM((block_cols, lane_tiles, LANES), jnp.float32),
            pltpu.SemaphoreType.DMA((4,)),
        ],
        compiler_params=pltpu.CompilerParams(vmem_limit_bytes=40 * 1024 * 1024),
        name="turn",
    )(
        jnp.where(remote, order, mates - first_col)[None, :],
        cosine,
        jnp.where(remote[None, :], 0.0, sine),
        tiles,
    )
    dest = spot // every
    dest_rank = jnp.sum(
        ((dest[:, None] == dest[None, :]) & (spot[None, :] < spot[:, None])).astype(jnp.int32),
        axis=1,
    )
    dest_slot = dest * move_cap + dest_rank
    places = dest_count * move_cap
    filled = dest_slot[None, :] == jnp.arange(places, dtype=jnp.int32)[:, None]
    place_source = one_hot_sum(filled, order)
    parcels = pl.pallas_call(
        functools.partial(pack_kernel, pieces),
        out_shape=jax.ShapeDtypeStruct((places, lane_tiles, LANES), jnp.float32),
        in_specs=[pl.BlockSpec(memory_space=pl.ANY)] * 3
        + [pl.BlockSpec(memory_space=pltpu.VMEM)] * 2,
        out_specs=pl.BlockSpec(memory_space=pl.ANY),
        scratch_shapes=[
            pltpu.SMEM((1, places), jnp.int32),
            pltpu.SMEM((1, block_cols), jnp.int32),
            pltpu.SMEM((1, block_cols), jnp.float32),
            pltpu.VMEM((places, lane_tiles, LANES), jnp.float32),
            pltpu.SemaphoreType.DMA((3,)),
            pltpu.SemaphoreType.DMA((pieces,)),
        ],
        compiler_params=pltpu.CompilerParams(vmem_limit_bytes=48 * 1024 * 1024),
        name="rotate_pack",
    )(place_source[None, :], mate_row[None, :], far_sine, turned, incoming)
    arrived = lax.all_to_all(
        parcels.reshape(dest_count, move_cap * lane_tiles, LANES),
        ("row", "col"), split_axis=0, concat_axis=0, tiled=True,
    )

    share = panel_cols // col_count
    zeros_here = lax.dynamic_slice_in_dim(secular_zeros, col_index * share, share)
    raw = secular_coefficients[:, None] / (secular_singularities[:, None] - zeros_here[None, :])
    scale = lax.rsqrt(jnp.sum(raw * raw, axis=0) + 1e-06)

    def shift(array, chip_step):
        pairs = [
            (2 * x + c, 2 * ((x + chip_step) % chips) + c) for x in range(chips) for c in range(2)
        ]
        return lax.ppermute(array, "col", pairs)

    swap = [(c, c ^ 1) for c in range(col_count)]
    partner = lax.ppermute(theirs, "col", swap)
    ours = ours.reshape(chips, share, block_rows)
    partner = partner.reshape(chips, share, block_rows)
    half = share // 2

    def pair(distance, rows):
        return ours[distance, rows] + partner[distance, rows]

    low, high = slice(0, half), slice(half, share)
    up = shift(jnp.concatenate([pair(2, low), pair(1, high)]), 1)
    down = shift(jnp.concatenate([pair(2, high), pair(3, low)]), -1)
    up_low = shift(pair(1, low) + up[:half], 1)
    down_high = shift(pair(3, high) + down[:half], -1)

    base = pair(0, slice(0, share)) + jnp.concatenate([down[half:], up[half:]])
    base = lax.optimization_barrier(base * scale[:, None])
    panel = base + jnp.concatenate([up_low, down_high]) * scale[:, None]
    arrived, panel = lax.optimization_barrier((arrived, panel))

    slot_index = lax.axis_index("row") * col_count + col_index
    wanted = lax.dynamic_slice_in_dim(kept_vectors, slot_index * every, every)
    source = wanted // block_cols
    earlier = jnp.arange(every, dtype=jnp.int32)
    source_rank = jnp.sum(
        ((source[:, None] == source[None, :]) & (earlier[None, :] < earlier[:, None])).astype(
            jnp.int32
        ),
        axis=1,
    )
    starts = source * move_cap + source_rank
    packed = pl.pallas_call(
        unpack_kernel,
        out_shape=jax.ShapeDtypeStruct(
            (every // SUB, row_count, lane_tiles * SUB, LANES), jnp.float32
        ),
        in_specs=[pl.BlockSpec(memory_space=pl.ANY)] * 2,
        out_specs=pl.BlockSpec(memory_space=pl.ANY),
        scratch_shapes=[
            pltpu.SMEM((1, every), jnp.int32),
            pltpu.VMEM((row_count, col_count * move_cap, lane_tiles, LANES), jnp.float32),
            pltpu.VMEM((every // SUB, row_count, lane_tiles * SUB, LANES), jnp.float32),
            pltpu.SemaphoreType.DMA,
            pltpu.SemaphoreType.DMA((pieces,)),
            pltpu.SemaphoreType.DMA((pieces,)),
        ],
        name="unpack",
    )(starts[None, :], arrived.reshape(row_count, col_count * move_cap, lane_tiles, LANES))
    packed_vectors = from_tiles(packed.reshape(-1, LANES), every, row_count * block_rows)
    return (packed_vectors, panel)


def solution(mesh):
    placed = (P("col", "row"), P(), P(), P(), P(), P(), P())

    return jax.shard_map(
        shards,
        mesh=mesh,
        in_specs=placed,
        out_specs=(P(("row", "col"), None), P("col", "row")),
        check_vma=False,
    )
```

```python
import functools

import jax
import jax.numpy as jnp
from jax import lax
from jax.experimental import pallas as pl
from jax.experimental.pallas import tpu as pltpu
from jax.sharding import PartitionSpec as P


LANES = 128
SUB = 8
GROUP = 8


def tile_view(rows):
    count, width = rows.shape
    tiles = rows.reshape(count // SUB, SUB, width // LANES, LANES).transpose(0, 2, 1, 3)
    return tiles.reshape(count // SUB, width // LANES * SUB, LANES)


def from_tiles(tiles, count, width):
    rows = tiles.reshape(count // SUB, width // LANES, SUB, LANES)
    return rows.transpose(0, 2, 1, 3).reshape(count, width)


def send_kernel(pair_cap, pieces, mates_hbm, tiles_hbm, out_hbm,
                mates_ref, tiles_ref, stage_ref, slots_ref, source_ref, sems):
    table = pltpu.make_async_copy(mates_hbm, mates_ref, sems.at[1])
    table.start()
    load = pltpu.make_async_copy(tiles_hbm, tiles_ref, sems.at[0])
    load.start()
    columns, parts = tiles_ref.shape[0] * SUB, stage_ref.shape[1] // SUB
    table.wait()
    count = stage_ref.shape[0]
    blocks = count // pair_cap
    local = columns // LANES
    local_mates = mates_ref[pl.ds(lax.axis_index("col") * local, local), :]
    owner = jnp.concatenate([local_mates[i : i + 1] for i in range(local)], axis=1) // columns
    member = lax.broadcasted_iota(jnp.int32, (blocks, columns), 0) == owner
    earlier = lax.broadcasted_iota(jnp.int32, (columns, columns), 0) < lax.broadcasted_iota(
        jnp.int32, (columns, columns), 1
    )
    before = jnp.dot(
        member.astype(jnp.bfloat16), earlier.astype(jnp.bfloat16),
        preferred_element_type=jnp.float32,
    )
    rank = jnp.sum(jnp.where(member, before, 0.0), axis=0, keepdims=True).astype(jnp.int32)
    place = jnp.where(rank < pair_cap, owner * pair_cap + rank, -1)
    pick = (
        lax.broadcasted_iota(jnp.int32, (count, columns), 0) == place
    ).astype(jnp.bfloat16)
    order = lax.broadcasted_iota(jnp.int32, (SUB, columns), 1)
    digit = lax.broadcasted_iota(jnp.int32, (SUB, columns), 0)
    digits = jnp.where(digit == 0, order // LANES, order % LANES).astype(jnp.bfloat16)
    found = lax.dot_general(
        digits, pick, (((1,), (1,)), ((), ())), preferred_element_type=jnp.float32
    )
    slots_ref[...] = (found[0:1] * LANES + found[1:2]).astype(jnp.int32)
    indices = pltpu.make_async_copy(slots_ref, source_ref, sems.at[1])
    indices.start()
    load.wait()

    indices.wait()

    def group(g, carry):
        values = []
        for n in range(GROUP):
            source = source_ref[0, g * GROUP + n]
            values += [
                tiles_ref[source // SUB, pl.ds(part * SUB * SUB + source % SUB, SUB, SUB), :]
                for part in range(parts)
            ]
        for n, value in enumerate(values):
            stage_ref[g * GROUP + n // parts, pl.ds(n % parts * SUB, SUB), :] = value
        return carry

    piece = count // pieces
    stores = []
    for n in range(pieces):
        lax.fori_loop(n * piece // GROUP, (n + 1) * piece // GROUP, group, 0, unroll=2)
        store = pltpu.make_async_copy(
            stage_ref.at[pl.ds(n * piece, piece)], out_hbm.at[pl.ds(n * piece, piece)], sems.at[2 + n]
        )
        store.start()
        stores.append(store)
    for store in stores:
        store.wait()


def split(value, parts):
    out = []
    for _ in range(parts):
        out.append(value.astype(jnp.bfloat16))
        value = value - out[-1].astype(jnp.float32)
    return out


def panel_kernel(mates_ref, theta_ref, kept_ref, pole_ref, weight_ref, zeros_ref, vec_hbm,
                 spot_ref, cos_ref, sin_ref, theirs_hbm, ours_hbm,
                 vec_ref, deep_ref, wide_high, wide_low, w_ref,
                 theirs_ref, ours_ref, load_sems, store_sems):
    chunks = load_sems.shape[0]
    columns, width = vec_ref.shape
    step = width // chunks
    loads = [
        pltpu.make_async_copy(
            vec_hbm.at[:, pl.ds(n * step, step)], vec_ref.at[:, pl.ds(n * step, step)],
            load_sems.at[n],
        )
        for n in range(chunks)
    ]
    for load in loads:
        load.start()

    total, groups, local = kept_ref.shape[1], mates_ref.shape[0], columns // LANES
    kept = kept_ref[...]
    row_hot = lax.broadcasted_iota(jnp.int32, (groups, total), 0) == kept // LANES
    lane_hot = (
        lax.broadcasted_iota(jnp.int32, (LANES, total), 0) == kept % LANES
    ).astype(jnp.bfloat16)
    place = lax.broadcasted_iota(jnp.int32, (1, total), 1)
    values = [(place // LANES).astype(jnp.float32), (place % LANES).astype(jnp.float32)]
    for ref in (pole_ref, weight_ref):
        values += [part.astype(jnp.float32) for part in split(ref[...], 3)]
    spread = jnp.concatenate([jnp.where(row_hot, value, 0.0) for value in values], axis=0)
    tables = lax.dot_general(
        spread.astype(jnp.bfloat16), lane_hot, (((1,), (1,)), ((), ())),
        preferred_element_type=jnp.float32,
    )
    tables = [tables[n * groups : (n + 1) * groups] for n in range(len(values))]
    tables += [part.astype(jnp.float32) for part in split(theta_ref[...], 3)]

    first = lax.axis_index("col")
    mine = (
        lax.broadcasted_iota(jnp.int32, (groups, LANES), 0) - first * local
    )

    def here(table):
        rows = [
            jnp.sum(jnp.where(mine == n, table, jnp.zeros((), table.dtype)), axis=0, keepdims=True)
            for n in range(local)
        ]
        return jnp.concatenate(rows, axis=1)

    mates = here(mates_ref[...])
    labels = first * columns + lax.broadcasted_iota(jnp.int32, (1, columns), 1)
    mate_lane = (
        lax.broadcasted_iota(jnp.int32, (LANES, columns), 0) == mates % LANES
    ).astype(jnp.bfloat16)
    mate_row = lax.broadcasted_iota(jnp.int32, (groups, columns), 0) == mates // LANES
    wanted = jnp.concatenate(tables[2:], axis=0).astype(jnp.bfloat16)
    picked = jnp.dot(wanted, mate_lane, preferred_element_type=jnp.float32)
    theirs = [
        jnp.sum(
            jnp.where(mate_row, picked[n * groups : (n + 1) * groups], 0.0), axis=0, keepdims=True
        )
        for n in range(9)
    ]
    mate_pole, mate_weight, mate_theta = [
        theirs[n] + (theirs[n + 1] + theirs[n + 2]) for n in (0, 3, 6)
    ]
    spot_ref[...] = here(tables[0] * LANES + tables[1]).astype(jnp.int32)
    pole = here(tables[2] + (tables[3] + tables[4]))
    weight = here(tables[5] + (tables[6] + tables[7]))
    angle = jnp.where(mates < labels, mate_theta, here(theta_ref[...]))
    paired = mates != labels
    cosine = jnp.where(paired, jnp.cos(angle), 1.0)
    sine = jnp.where(paired, jnp.where(labels < mates, -1.0, 1.0) * jnp.sin(angle), 0.0)
    cos_ref[...] = cosine
    sin_ref[...] = sine

    own_part, mate_part = cosine * weight, sine * mate_weight
    for q in range(zeros_ref.shape[0]):
        zeros = jnp.broadcast_to(zeros_ref[q : q + 1], (LANES, LANES)).T
        for t in range(local):
            at = slice(t * LANES, (t + 1) * LANES)
            value = own_part[:, at] / (pole[:, at] - zeros) - mate_part[:, at] / (
                mate_pole[:, at] - zeros
            )
            high, low = split(value, 2)
            wide_high[q * LANES : (q + 1) * LANES, at] = high
            wide_low[q * LANES : (q + 1) * LANES, at] = low

    half = theirs_ref.shape[0]
    block = half // 4
    chip, core = first // 2, first % 2
    count = half // block
    for parity in range(2):
        for distance in range(count):
            owner = (chip + distance) % count * 2 + (1 - core if parity == 0 else core)
            source = pl.ds(pl.multiple_of(owner * block, block), block)
            target = slice(parity * half + distance * block, parity * half + (distance + 1) * block)
            w_ref[target, 0:columns] = wide_high[source, :]
            w_ref[target, columns : 2 * columns] = wide_high[source, :]
            w_ref[target, 2 * columns :] = wide_low[source, :]

    stores = []
    for parity, (stage, out) in enumerate(((theirs_ref, theirs_hbm), (ours_ref, ours_hbm))):
        rows = slice(parity * half, (parity + 1) * half)
        for n in range(chunks):
            at = slice(n * step, (n + 1) * step)
            if parity == 0:
                loads[n].wait()
                high, low = split(vec_ref[:, at], 2)
                deep_ref[0:columns, at] = high
                deep_ref[columns : 2 * columns, at] = low
                deep_ref[2 * columns :, at] = high
            stage[:, at] = jnp.dot(
                w_ref[rows, :], deep_ref[:, at], preferred_element_type=jnp.float32
            )
            part = pl.ds(n * step, step)
            store = pltpu.make_async_copy(
                stage.at[:, part], out.at[:, part], store_sems.at[parity * chunks + n]
            )
            store.start()
            stores.append(store)
    for store in stores:
        store.wait()


def turn_kernel(mate_hbm, cos_hbm, sin_hbm, tiles_hbm, turned_ref,
                mate_ref, cos_ref, sin_ref, tiles_ref, rows_ref, sems):
    loads = [
        pltpu.make_async_copy(source, ref, sems.at[n])
        for n, (source, ref) in enumerate((
            (tiles_hbm, tiles_ref), (mate_hbm, mate_ref), (cos_hbm, cos_ref), (sin_hbm, sin_ref)
        ))
    ]
    for load in loads:
        load.start()
    loads[0].wait()
    parts = rows_ref.shape[1] // SUB

    def spread(g, carry):
        values = [
            tiles_ref[g, pl.ds(part * SUB * SUB + s, SUB, SUB), :]
            for s in range(SUB) for part in range(parts)
        ]
        for n, value in enumerate(values):
            rows_ref[g * SUB + n // parts, pl.ds(n % parts * SUB, SUB), :] = value
        return carry

    lax.fori_loop(0, tiles_ref.shape[0], spread, 0, unroll=2)
    for load in loads[1:]:
        load.wait()

    def turn(g, carry):
        columns = [g * GROUP + n for n in range(GROUP)]
        values = [
            cos_ref[0, i] * rows_ref[i] + sin_ref[0, i] * rows_ref[mate_ref[0, i]] for i in columns
        ]
        for i, value in zip(columns, values):
            turned_ref[i] = value
        return carry

    lax.fori_loop(0, rows_ref.shape[0] // GROUP, turn, 0, unroll=2)


def pack_kernel(pieces, source_hbm, mate_hbm, sin_hbm, turned_ref, mates_hbm, out_hbm,
                source_ref, mate_ref, sin_ref, mates_ref, stage_ref, load_sems, store_sems):
    tables = [
        pltpu.make_async_copy(table, ref, load_sems.at[n])
        for n, (table, ref) in enumerate(
            (
                (mates_hbm, mates_ref), (source_hbm, source_ref),
                (mate_hbm, mate_ref), (sin_hbm, sin_ref),
            )
        )
    ]
    for table in tables:
        table.start()
    for table in tables:
        table.wait()

    def group(g, carry):
        sources = [source_ref[0, g * GROUP + n] for n in range(GROUP)]
        values = [turned_ref[i] + sin_ref[0, i] * mates_ref[mate_ref[0, i]] for i in sources]
        for n, value in enumerate(values):
            stage_ref[g * GROUP + n] = value
        return carry

    piece = stage_ref.shape[0] // pieces
    stores = []
    for n in range(pieces):
        lax.fori_loop(n * piece // GROUP, (n + 1) * piece // GROUP, group, 0, unroll=2)
        part = pl.ds(n * piece, piece)
        store = pltpu.make_async_copy(stage_ref.at[part], out_hbm.at[part], store_sems.at[n])
        store.start()
        stores.append(store)
    for store in stores:
        store.wait()


def unpack_kernel(start_hbm, in_hbm, out_hbm, start_ref, in_ref, out_ref,
                  table_sem, load_sems, store_sems):
    pieces = load_sems.shape[0]
    rows, parts = in_ref.shape[0], in_ref.shape[2] // SUB
    wanted, per = start_ref.shape[1], rows // pieces
    table = pltpu.make_async_copy(start_hbm, start_ref, table_sem)
    table.start()
    loads, stores = [], []
    for n in range(pieces):
        part = pl.ds(n * per, per)
        loads.append(pltpu.make_async_copy(in_hbm.at[part], in_ref.at[part], load_sems.at[n]))
        stores.append(
            pltpu.make_async_copy(out_ref.at[:, part], out_hbm.at[:, part], store_sems.at[n])
        )
        loads[n].start()
    table.wait()
    for n in range(pieces):
        loads[n].wait()

        def row(r, carry):
            for first in range(0, wanted, SUB):
                values = [in_ref[r, start_ref[0, first + k]] for k in range(SUB)]
                for k, value in enumerate(values):
                    for part in range(parts):
                        out_ref[first // SUB, r, pl.ds(part * SUB * SUB + k, SUB, SUB), :] = value[
                            part * SUB : (part + 1) * SUB
                        ]
            return carry

        lax.fori_loop(n * per, (n + 1) * per, row, 0)
        stores[n].start()
    for store in stores:
        store.wait()


def one_hot_sum(match, values):
    return jnp.sum(jnp.where(match, values[None, :], jnp.zeros((), values.dtype)), axis=1)


def shards(
    eigvec_halves,
    rotation_mate,
    givens_theta,
    kept_vectors,
    secular_singularities,
    secular_coefficients,
    secular_zeros,
):
    col_count = lax.axis_size("col")
    row_count = lax.axis_size("row")
    chips = col_count // 2
    block_cols, block_rows = eigvec_halves.shape
    total_cols = rotation_mate.shape[0]
    panel_cols = secular_zeros.shape[0]
    pair_cap = block_cols // 16
    lane_tiles = block_rows // LANES
    dest_count = row_count * col_count
    every = total_cols // dest_count
    move_cap = every // col_count + every // col_count // 3
    col_index = lax.axis_index("col")
    first_col = col_index * block_cols

    order = jnp.arange(block_cols, dtype=jnp.int32)
    mates = lax.dynamic_slice_in_dim(rotation_mate, first_col, block_cols)
    owner = mates // block_cols
    same_owner = owner[:, None] == owner[None, :]
    tiles = tile_view(eigvec_halves)
    slot_count = col_count * pair_cap
    pieces = 4
    outgoing = pl.pallas_call(
        functools.partial(send_kernel, pair_cap, 2 * pieces),
        out_shape=jax.ShapeDtypeStruct((slot_count, lane_tiles, LANES), jnp.float32),
        in_specs=[pl.BlockSpec(memory_space=pl.ANY)] * 2,
        out_specs=pl.BlockSpec(memory_space=pl.ANY),
        scratch_shapes=[
            pltpu.VMEM((total_cols // LANES, LANES), jnp.int32),
            pltpu.VMEM(tiles.shape, jnp.float32),
            pltpu.VMEM((slot_count, lane_tiles, LANES), jnp.float32),
            pltpu.VMEM((1, slot_count), jnp.int32),
            pltpu.SMEM((1, slot_count), jnp.int32),
            pltpu.SemaphoreType.DMA((2 + 2 * pieces,)),
        ],
        name="send",
    )(rotation_mate.reshape(-1, LANES), tiles)
    incoming = lax.all_to_all(outgoing, "col", split_axis=0, concat_axis=0, tiled=True)

    half_cols = panel_cols // 2
    vec_chunks = 2
    spot, cosine, sine, theirs, ours = pl.pallas_call(
        panel_kernel,
        out_shape=[
            jax.ShapeDtypeStruct((1, block_cols), jnp.int32),
            jax.ShapeDtypeStruct((1, block_cols), jnp.float32),
            jax.ShapeDtypeStruct((1, block_cols), jnp.float32),
            jax.ShapeDtypeStruct((half_cols, block_rows), jnp.float32),
            jax.ShapeDtypeStruct((half_cols, block_rows), jnp.float32),
        ],
        in_specs=[pl.BlockSpec(memory_space=pltpu.VMEM)] * 6
        + [pl.BlockSpec(memory_space=pl.ANY)],
        out_specs=[pl.BlockSpec(memory_space=pltpu.VMEM)] * 3
        + [pl.BlockSpec(memory_space=pl.ANY)] * 2,
        scratch_shapes=[
            pltpu.VMEM((block_cols, block_rows), jnp.float32),
            pltpu.VMEM((3 * block_cols, block_rows), jnp.bfloat16),
            pltpu.VMEM((panel_cols, block_cols), jnp.bfloat16),
            pltpu.VMEM((panel_cols, block_cols), jnp.bfloat16),
            pltpu.VMEM((panel_cols, 3 * block_cols), jnp.bfloat16),
            pltpu.VMEM((half_cols, block_rows), jnp.float32),
            pltpu.VMEM((half_cols, block_rows), jnp.float32),
            pltpu.SemaphoreType.DMA((vec_chunks,)),
            pltpu.SemaphoreType.DMA((2 * vec_chunks,)),
        ],
        name="panel",
    )(
        rotation_mate.reshape(-1, LANES),
        givens_theta.reshape(-1, LANES),
        kept_vectors[None, :],
        secular_singularities[None, :],
        secular_coefficients[None, :],
        secular_zeros.reshape(-1, LANES),
        eigvec_halves,
    )
    spot = spot[0]
    recv_rank = jnp.sum((same_owner & (mates[None, :] < mates[:, None])).astype(jnp.int32), axis=1)
    remote = owner != col_index
    mate_row = jnp.where(remote, owner * pair_cap + recv_rank, 0)
    far_sine = jnp.where(remote[None, :], sine, 0.0)
    turned = pl.pallas_call(
        turn_kernel,
        out_shape=pltpu.VMEM((block_cols, lane_tiles, LANES), jnp.float32),
        in_specs=[pl.BlockSpec(memory_space=pl.ANY)] * 4,
        out_specs=pl.BlockSpec(memory_space=pltpu.VMEM),
        scratch_shapes=[
            pltpu.SMEM((1, block_cols), jnp.int32),
            pltpu.SMEM((1, block_cols), jnp.float32),
            pltpu.SMEM((1, block_cols), jnp.float32),
            pltpu.VMEM(tiles.shape, jnp.float32),
            pltpu.VMEM((block_cols, lane_tiles, LANES), jnp.float32),
            pltpu.SemaphoreType.DMA((4,)),
        ],
        compiler_params=pltpu.CompilerParams(vmem_limit_bytes=40 * 1024 * 1024),
        name="turn",
    )(
        jnp.where(remote, order, mates - first_col)[None, :],
        cosine,
        jnp.where(remote[None, :], 0.0, sine),
        tiles,
    )
    dest = spot // every
    dest_rank = jnp.sum(
        ((dest[:, None] == dest[None, :]) & (spot[None, :] < spot[:, None])).astype(jnp.int32),
        axis=1,
    )
    dest_slot = dest * move_cap + dest_rank
    places = dest_count * move_cap
    filled = dest_slot[None, :] == jnp.arange(places, dtype=jnp.int32)[:, None]
    place_source = one_hot_sum(filled, order)
    parcels = pl.pallas_call(
        functools.partial(pack_kernel, 2 * pieces),
        out_shape=jax.ShapeDtypeStruct((places, lane_tiles, LANES), jnp.float32),
        in_specs=[pl.BlockSpec(memory_space=pl.ANY)] * 3
        + [pl.BlockSpec(memory_space=pltpu.VMEM), pl.BlockSpec(memory_space=pl.ANY)],
        out_specs=pl.BlockSpec(memory_space=pl.ANY),
        scratch_shapes=[
            pltpu.SMEM((1, places), jnp.int32),
            pltpu.SMEM((1, block_cols), jnp.int32),
            pltpu.SMEM((1, block_cols), jnp.float32),
            pltpu.VMEM((slot_count, lane_tiles, LANES), jnp.float32),
            pltpu.VMEM((places, lane_tiles, LANES), jnp.float32),
            pltpu.SemaphoreType.DMA((4,)),
            pltpu.SemaphoreType.DMA((2 * pieces,)),
        ],
        compiler_params=pltpu.CompilerParams(vmem_limit_bytes=48 * 1024 * 1024),
        name="rotate_pack",
    )(place_source[None, :], mate_row[None, :], far_sine, turned, incoming)
    arrived = lax.all_to_all(
        parcels.reshape(dest_count, move_cap * lane_tiles, LANES),
        ("row", "col"), split_axis=0, concat_axis=0, tiled=True,
    )

    share = panel_cols // col_count
    zeros_here = lax.dynamic_slice_in_dim(secular_zeros, col_index * share, share)
    raw = secular_coefficients[:, None] / (secular_singularities[:, None] - zeros_here[None, :])
    scale = lax.rsqrt(jnp.sum(raw * raw, axis=0) + 1e-06)

    def shift(array, chip_step):
        pairs = [
            (2 * x + c, 2 * ((x + chip_step) % chips) + c) for x in range(chips) for c in range(2)
        ]
        return lax.ppermute(array, "col", pairs)

    swap = [(c, c ^ 1) for c in range(col_count)]
    partner = lax.ppermute(theirs, "col", swap)
    ours = ours.reshape(chips, share, block_rows)
    partner = partner.reshape(chips, share, block_rows)
    half = share // 2

    def pair(distance, rows):
        return ours[distance, rows] + partner[distance, rows]

    low, high = slice(0, half), slice(half, share)
    up = shift(jnp.concatenate([pair(2, low), pair(1, high)]), 1)
    down = shift(jnp.concatenate([pair(2, high), pair(3, low)]), -1)
    up_low = shift(pair(1, low) + up[:half], 1)
    down_high = shift(pair(3, high) + down[:half], -1)

    base = pair(0, slice(0, share)) + jnp.concatenate([down[half:], up[half:]])
    base = lax.optimization_barrier(base * scale[:, None])
    panel = base + jnp.concatenate([up_low, down_high]) * scale[:, None]
    arrived, panel = lax.optimization_barrier((arrived, panel))

    slot_index = lax.axis_index("row") * col_count + col_index
    wanted = lax.dynamic_slice_in_dim(kept_vectors, slot_index * every, every)
    source = wanted // block_cols
    earlier = jnp.arange(every, dtype=jnp.int32)
    source_rank = jnp.sum(
        ((source[:, None] == source[None, :]) & (earlier[None, :] < earlier[:, None])).astype(
            jnp.int32
        ),
        axis=1,
    )
    starts = source * move_cap + source_rank
    packed = pl.pallas_call(
        unpack_kernel,
        out_shape=jax.ShapeDtypeStruct(
            (every // SUB, row_count, lane_tiles * SUB, LANES), jnp.float32
        ),
        in_specs=[pl.BlockSpec(memory_space=pl.ANY)] * 2,
        out_specs=pl.BlockSpec(memory_space=pl.ANY),
        scratch_shapes=[
            pltpu.SMEM((1, every), jnp.int32),
            pltpu.VMEM((row_count, col_count * move_cap, lane_tiles, LANES), jnp.float32),
            pltpu.VMEM((every // SUB, row_count, lane_tiles * SUB, LANES), jnp.float32),
            pltpu.SemaphoreType.DMA,
            pltpu.SemaphoreType.DMA((pieces,)),
            pltpu.SemaphoreType.DMA((pieces,)),
        ],
        name="unpack",
    )(starts[None, :], arrived.reshape(row_count, col_count * move_cap, lane_tiles, LANES))
    packed_vectors = from_tiles(packed.reshape(-1, LANES), every, row_count * block_rows)
    return (packed_vectors, panel)


def solution(mesh):
    placed = (P("col", "row"), P(), P(), P(), P(), P(), P())

    return jax.shard_map(
        shards,
        mesh=mesh,
        in_specs=placed,
        out_specs=(P(("row", "col"), None), P("col", "row")),
        check_vma=False,
    )
```
